8 devices in a mesh: dp: 8 (over z, y, x, core).
Axes of the slice: x: 2, y: 2, z: 1, core: 2. Of those that a mesh axis runs over, the one named last changes fastest.
Arguments:
- g_mat: bfloat16 [8, 19660800], P('dp')
- g_vec: bfloat16 [8, 24320], P('dp')
- p_mat: float32 [19660800], P('dp')
- m_mat: float32 [19660800], P('dp')
- v_mat: float32 [19660800], P('dp')
- p_vec: float32 [24320], replicated
- m_vec: float32 [24320], replicated
- v_vec: float32 [24320], replicated
- learn_rate: float32 [], replicated
Outputs:
- output 1: float32 [19660800], P('dp')
- output 2: float32 [19660800], P('dp')
- output 3: float32 [19660800], P('dp')
- output 4: float32 [24320], replicated
- output 5: float32 [24320], replicated
- output 6: float32 [24320], replicated
- output 7: bfloat16 [19660800], replicated
All inputs are finite; a program needn't handle non-finite values.
Results may differ from the reference program's by a relative error of at most 0.001.
Values are sent between devices in bfloat16 or wider.
A program may use at most 1 GiB of HBM per device.

```python
import jax
import jax.numpy as jnp
from jax import lax

D = 1280
FF = 5120
TP = 2
DP = 8
STEP = 10

N_MAT = (8 * D * D + 4 * D * FF) // TP
N_VEC = 2 * ((3 * D + FF) // TP) + 12 * D
N_ALL = N_MAT + N_VEC
ELEM_SCALE = N_ALL ** -0.5
NOISE_GAIN = 6.0 * DP ** 0.5
ADAM_BETA1 = 0.9
ADAM_BETA2 = 0.98
ADAM_EPS = 1e-8
WEIGHT_DECAY = 0.01
MAX_NORM = 1.0
NORM_EPS = 1e-6
BIAS_ONE = 1.0 - ADAM_BETA1 ** STEP
BIAS_TWO = 1.0 - ADAM_BETA2 ** STEP


def draw_local_grads(draw_key, elem_count):
    key_base, key_dev = jax.random.split(draw_key)
    base_part = 2.0 * jax.random.normal(key_base, (elem_count,), jnp.float32)
    dev_keys = jax.random.split(key_dev, DP)

    def one_device(dev_key):
        noise_part = jax.random.normal(dev_key, (elem_count,), jnp.float32)
        return ((base_part + NOISE_GAIN * noise_part) * ELEM_SCALE).astype(jnp.bfloat16)

    return lax.map(one_device, dev_keys)


def setup_inputs(seed: int = 0) -> dict:
    key_list = jax.random.split(jax.random.key(seed), 9)
    return dict(
        g_mat=draw_local_grads(key_list[0], N_MAT),
        g_vec=draw_local_grads(key_list[1], N_VEC),
        p_mat=0.02 * jax.random.normal(key_list[2], (N_MAT,), jnp.float32),
        m_mat=0.1 * ELEM_SCALE * jax.random.normal(key_list[3], (N_MAT,), jnp.float32),
        v_mat=0.05 * ELEM_SCALE * ELEM_SCALE * jax.random.uniform(key_list[4], (N_MAT,), jnp.float32, minval=0.25, maxval=1.75),
        p_vec=0.05 * jax.random.normal(key_list[5], (N_VEC,), jnp.float32),
        m_vec=0.1 * ELEM_SCALE * jax.random.normal(key_list[6], (N_VEC,), jnp.float32),
        v_vec=0.05 * ELEM_SCALE * ELEM_SCALE * jax.random.uniform(key_list[7], (N_VEC,), jnp.float32, minval=0.25, maxval=1.75),
        learn_rate=jax.random.uniform(key_list[8], (), jnp.float32, minval=0.002, maxval=0.008),
    )


def mean_over_devices(local_grads):
    def add_row(acc_sum, grad_row):
        return acc_sum + grad_row.astype(jnp.float32), None

    total_sum, _ = lax.scan(add_row, jnp.zeros(local_grads.shape[1:], jnp.float32), local_grads)
    return total_sum / local_grads.shape[0]


def adam_update(grad_vals, param_vals, moment_one, moment_two, learn_rate, decay_rate):
    new_one = ADAM_BETA1 * moment_one + (1.0 - ADAM_BETA1) * grad_vals
    new_two = ADAM_BETA2 * moment_two + (1.0 - ADAM_BETA2) * grad_vals * grad_vals
    direction = (new_one / BIAS_ONE) / (jnp.sqrt(new_two / BIAS_TWO) + ADAM_EPS)
    return param_vals - learn_rate * (direction + decay_rate * param_vals), new_one, new_two


def reference(g_mat, g_vec, p_mat, m_mat, v_mat, p_vec, m_vec, v_vec, learn_rate):
    grad_mat = mean_over_devices(g_mat)
    grad_vec = mean_over_devices(g_vec)
    norm_sq = jnp.sum(grad_mat * grad_mat) + jnp.sum(grad_vec * grad_vec)
    clip_scale = jnp.minimum(1.0, MAX_NORM / (jnp.sqrt(norm_sq) + NORM_EPS))
    new_p_mat, new_m_mat, new_v_mat = adam_update(grad_mat * clip_scale, p_mat, m_mat, v_mat, learn_rate, WEIGHT_DECAY)
    new_p_vec, new_m_vec, new_v_vec = adam_update(grad_vec * clip_scale, p_vec, m_vec, v_vec, learn_rate, 0.0)
    return (new_p_mat, new_m_mat, new_v_mat, new_p_vec, new_m_vec, new_v_vec, new_p_mat.astype(jnp.bfloat16))
```

```python
import functools

import jax
import jax.numpy as jnp
from jax import lax
from jax.experimental import pallas as pl
from jax.experimental.pallas import tpu as pltpu
from jax.sharding import PartitionSpec as P

STEP = 10
ADAM_BETA1 = 0.9
ADAM_BETA2 = 0.98
ADAM_EPS = 1e-8
WEIGHT_DECAY = 0.01
MAX_NORM = 1.0
NORM_EPS = 1e-6
BIAS_ONE = 1.0 - ADAM_BETA1 ** STEP
BIAS_TWO = 1.0 - ADAM_BETA2 ** STEP

MESH = pl.DeviceIdType.MESH
LANES = 128
DEVICES = 8
CHUNKS = 10
BLOCK = 96


def adam_update(grad_vals, param_vals, moment_one, moment_two, learn_rate, decay_rate):
    new_one = ADAM_BETA1 * moment_one + (1.0 - ADAM_BETA1) * grad_vals
    new_two = ADAM_BETA2 * moment_two + (1.0 - ADAM_BETA2) * grad_vals * grad_vals
    direction = (new_one / BIAS_ONE) / (jnp.sqrt(new_two / BIAS_TWO) + ADAM_EPS)
    return param_vals - learn_rate * (direction + decay_rate * param_vals), new_one, new_two


def places(axis_name):
    me = lax.axis_index(axis_name)
    core, x, y = me % 2, (me // 2) % 2, me // 4

    def dev(yy, xx, cc):
        return 4 * yy + 2 * xx + cc

    return me, core, x, y, dev


def reduce_kernel(axis_name, half_rows, g_ref, gv_ref, gsum_ref, vsum_ref, clip_ref, stage_ref,
                  first, own_first, direct, own_direct, fsum, psum, raw, packed, vrecv, nsend, nrecv,
                  raw_sem, pack_sem, first_recv, direct_recv, psum_recv, send_sem, fsum_send,
                  vec_send, vec_recv, nrm_send, nrm_recv, out_sem):
    me, core, x, y, dev = places(axis_name)
    sib = dev(y, x, 1 - core)
    xs = [dev(y, 1 - x, 0), dev(y, 1 - x, 1)]
    ys = [dev(1 - y, x, 0), dev(1 - y, x, 1)]
    ds = [dev(1 - y, 1 - x, 0), dev(1 - y, 1 - x, 1)]
    x_mine, x_sib = dev(y, 1 - x, core), dev(y, 1 - x, 1 - core)
    y_mine, y_sib = dev(1 - y, x, core), dev(1 - y, x, 1 - core)
    rows = half_rows // CHUNKS
    vals = rows * LANES

    first_plan = [
        (2 * ds[0], ys[0], first, (0, core), first_recv),
        (2 * ds[0] + 1, xs[0], first, (1, core), first_recv),
        (2 * ds[1], ys[1], first, (0, core), first_recv),
        (2 * ds[1] + 1, xs[1], first, (1, core), first_recv),
        (2 * x_sib, sib, first, (0, 2), first_recv),
        (2 * y_sib + 1, sib, first, (1, 2), first_recv),
        (2 * x_mine, None, own_first, (0,), None),
        (2 * y_mine + 1, None, own_first, (1,), None),
    ]
    direct_plan = [
        (2 * ys[0], ys[0], direct, (0, core), direct_recv),
        (2 * xs[0] + 1, xs[0], direct, (1, core), direct_recv),
        (2 * ys[1], ys[1], direct, (0, core), direct_recv),
        (2 * xs[1] + 1, xs[1], direct, (1, core), direct_recv),
        (2 * sib, sib, direct, (0, 2), direct_recv),
        (2 * sib + 1, sib, direct, (1, 2), direct_recv),
        (2 * me, None, own_direct, (0,), None),
        (2 * me + 1, None, own_direct, (1,), None),
    ]

    def load_raw(plan, h, c):
        start = pl.multiple_of((plan[h][0] * CHUNKS + c) * vals, vals)
        return pltpu.make_async_copy(g_ref.at[:, pl.ds(start, vals)], raw.at[h], raw_sem.at[h])

    def stage_at(phase, h, c):
        return stage_ref.at[6 * phase + h, pl.ds(pl.multiple_of(c * rows, rows), rows), :]

    def to_stage(phase, h, c):
        return pltpu.make_async_copy(packed.at[h], stage_at(phase, h, c), pack_sem.at[h])

    def send(phase, plan, h, c):
        _, target, buf, slot, sems = plan[h]
        return pltpu.make_async_remote_copy(
            src_ref=stage_at(phase, h, c),
            dst_ref=buf.at[(*slot, pl.ds(pl.multiple_of(c * rows, rows), rows))],
            send_sem=send_sem.at[6 * phase + h, c],
            recv_sem=sems.at[(*slot, c)],
            device_id=(target,),
            device_id_type=MESH,
        )

    def pack(plan, h, c):
        _, target, buf, slot, _ = plan[h]

        def body(i, _):
            piece = raw[h, :, pl.ds(pl.multiple_of(i * BLOCK * LANES, BLOCK * LANES), BLOCK * LANES)]
            piece = piece.astype(jnp.float32).reshape(BLOCK, LANES).astype(jnp.bfloat16)
            if target is None:
                buf[(*slot, pl.ds(pl.multiple_of(c * rows + i * BLOCK, BLOCK), BLOCK), slice(None))] = piece
            else:
                packed[h, pl.ds(pl.multiple_of(i * BLOCK, BLOCK), BLOCK), :] = piece
            return 0

        lax.fori_loop(0, rows // BLOCK, body, 0)

    for h in range(8):
        load_raw(first_plan, h, 0).start()

    vrecv[me] = gv_ref[...]

    barrier = pltpu.get_barrier_semaphore()
    for o in range(1, DEVICES):
        pl.semaphore_signal(barrier, inc=1, device_id=((me + o) % DEVICES,), device_id_type=MESH)
    pl.semaphore_wait(barrier, DEVICES - 1)

    def vec_copy(o):
        return pltpu.make_async_remote_copy(
            src_ref=gv_ref, dst_ref=vrecv.at[me], send_sem=vec_send.at[o], recv_sem=vec_recv.at[me],
            device_id=((me + o) % DEVICES,), device_id_type=MESH)

    def vec_wait(o):
        src = (me + o) % DEVICES
        pltpu.make_async_copy(gv_ref, vrecv.at[src], vec_recv.at[src]).wait()

    for o in range(1, DEVICES):
        vec_copy(o).start()

    def send_phase(phase, plan, next_plan):
        def step(c, _):
            for h in range(8):
                load_raw(plan, h, c).wait()
                pack(plan, h, c)
                if next_plan is None:
                    @pl.when(c + 1 < CHUNKS)
                    def _():
                        load_raw(plan, h, c + 1).start()
                else:
                    @pl.when(c + 1 < CHUNKS)
                    def _():
                        load_raw(plan, h, c + 1).start()

                    @pl.when(c + 1 >= CHUNKS)
                    def _():
                        load_raw(next_plan, h, 0).start()
                if 1 <= h <= 6:
                    to_stage(phase, h - 1, c).start()
            for h in range(6):
                to_stage(phase, h, c).wait()
                send(phase, plan, h, c).start()
            return 0

        lax.fori_loop(0, CHUNKS, step, 0)

    send_phase(0, first_plan, direct_plan)
    send_phase(1, direct_plan, None)

    def got(buf, sems, slot, c):
        at = buf.at[(*slot, pl.ds(pl.multiple_of(c * rows, rows), rows))]
        pltpu.make_async_copy(at, at, sems.at[(*slot, c)]).wait()

    def fsum_copy(side, c):
        at = (side, pl.ds(pl.multiple_of(c * rows, rows), rows))
        return pltpu.make_async_remote_copy(
            src_ref=fsum.at[at], dst_ref=psum.at[at], send_sem=fsum_send.at[side, c], recv_sem=psum_recv.at[side, c],
            device_id=((x_mine, y_mine)[side],), device_id_type=MESH)

    def relay_step(c, _):
        for side in range(2):
            for slot in range(3):
                got(first, first_recv, (side, slot), c)

            def body(i, _, side=side):
                at = pl.ds(pl.multiple_of(c * rows + i * BLOCK, BLOCK), BLOCK)
                total = first[side, 0, at, :].astype(jnp.float32) + first[side, 1, at, :].astype(jnp.float32)
                total = total + (first[side, 2, at, :].astype(jnp.float32) + own_first[side, at, :].astype(jnp.float32))
                fsum[side, at, :] = total
                return 0

            lax.fori_loop(0, rows // BLOCK, body, 0)
            if side == 1:
                fsum_copy(0, c).start()
            else:
                @pl.when(c > 0)
                def _():
                    fsum_copy(1, c - 1).start()
        return 0

    lax.fori_loop(0, CHUNKS, relay_step, 0)

    for o in range(1, DEVICES):
        vec_wait(o)
    vec_total = vrecv[0].astype(jnp.float32)
    for d in range(1, DEVICES):
        vec_total = vec_total + vrecv[d].astype(jnp.float32)
    vec_mean = vec_total / DEVICES
    vsum_ref[...] = vec_mean
    fsum_copy(1, CHUNKS - 1).start()

    def out_copy(side, c):
        at = pl.ds(pl.multiple_of(c * rows, rows), rows)
        to = pl.ds(pl.multiple_of(side * half_rows + c * rows, rows), rows)
        return pltpu.make_async_copy(psum.at[side, at], gsum_ref.at[to], out_sem.at[side, c])

    def final_step(c, acc):
        for side in range(2):
            got(psum, psum_recv, (side,), c)
            for slot in range(3):
                got(direct, direct_recv, (side, slot), c)

            def body(i, acc, side=side):
                at = pl.ds(pl.multiple_of(c * rows + i * BLOCK, BLOCK), BLOCK)
                total = direct[side, 0, at, :].astype(jnp.float32) + direct[side, 1, at, :].astype(jnp.float32)
                total = total + (direct[side, 2, at, :].astype(jnp.float32) + own_direct[side, at, :].astype(jnp.float32))
                mean = (psum[side, at, :] + total) / DEVICES
                psum[side, at, :] = mean
                return acc + jnp.sum((mean * mean).reshape(BLOCK // 8, 8, LANES), axis=0)

            acc = lax.fori_loop(0, rows // BLOCK, body, acc)
            if side == 1:
                out_copy(0, c).start()
            else:
                @pl.when(c > 0)
                def _():
                    out_copy(1, c - 1).start()
        return acc

    acc = lax.fori_loop(0, CHUNKS, final_step, jnp.zeros((8, LANES), jnp.float32))
    nsend[...] = acc
    nrecv[me] = acc
    out_copy(1, CHUNKS - 1).start()

    def drain(c, _):
        for h in range(6):
            send(0, first_plan, h, c).wait_send()
            send(1, direct_plan, h, c).wait_send()
        return 0

    lax.fori_loop(0, CHUNKS, drain, 0)

    def nrm_copy(o):
        return pltpu.make_async_remote_copy(
            src_ref=nsend, dst_ref=nrecv.at[me], send_sem=nrm_send.at[o], recv_sem=nrm_recv.at[me],
            device_id=((me + o) % DEVICES,), device_id_type=MESH)

    def nrm_wait(o):
        src = (me + o) % DEVICES
        pltpu.make_async_copy(nsend, nrecv.at[src], nrm_recv.at[src]).wait()

    for o in range(1, DEVICES):
        nrm_copy(o).start()

    def drain_rest(c, _):
        for side in range(2):
            fsum_copy(side, c).wait_send()
            out_copy(side, c).wait()
        return 0

    lax.fori_loop(0, CHUNKS, drain_rest, 0)
    for o in range(1, DEVICES):
        vec_copy(o).wait_send()
    for o in range(1, DEVICES):
        nrm_wait(o)
    tile = jnp.sum((vec_mean * vec_mean).reshape(-1, 8, LANES), axis=0)
    for d in range(DEVICES):
        tile = tile + nrecv[d]
    norm_sq = jnp.full((8, LANES), jnp.sum(tile), jnp.float32)
    clip_ref[...] = jnp.minimum(1.0, MAX_NORM / (jnp.sqrt(norm_sq) + NORM_EPS))
    for o in range(1, DEVICES):
        nrm_copy(o).wait_send()


def reduce_gradients(axis_name, g_mat, g_vec_rows):
    half_rows = g_mat.shape[1] // (2 * DEVICES * LANES)
    rows = half_rows // CHUNKS
    vec_rows = g_vec_rows.shape[0]
    bf16, f32 = jnp.bfloat16, jnp.float32
    dma = pltpu.SemaphoreType.DMA
    hbm, vmem = pl.BlockSpec(memory_space=pltpu.HBM), pl.BlockSpec(memory_space=pltpu.VMEM)
    return pl.pallas_call(
        functools.partial(reduce_kernel, axis_name, half_rows),
        out_shape=(
            jax.ShapeDtypeStruct((2 * half_rows, LANES), f32),
            jax.ShapeDtypeStruct((vec_rows, LANES), f32),
            jax.ShapeDtypeStruct((8, LANES), f32),
            jax.ShapeDtypeStruct((12, half_rows, LANES), bf16),
        ),
        in_specs=[hbm, vmem],
        out_specs=(hbm, vmem, vmem, hbm),
        scratch_shapes=[
            pltpu.VMEM((2, 3, half_rows, LANES), bf16),
            pltpu.VMEM((2, half_rows, LANES), bf16),
            pltpu.VMEM((2, 3, half_rows, LANES), bf16),
            pltpu.VMEM((2, half_rows, LANES), bf16),
            pltpu.VMEM((2, half_rows, LANES), f32),
            pltpu.VMEM((2, half_rows, LANES), f32),
            pltpu.VMEM((8, 1, rows * LANES), bf16),
            pltpu.VMEM((6, rows, LANES), bf16),
            pltpu.VMEM((DEVICES, vec_rows, LANES), bf16),
            pltpu.VMEM((8, LANES), f32),
            pltpu.VMEM((DEVICES, 8, LANES), f32),
            dma((8,)),
            dma((6,)),
            dma((2, 3, CHUNKS)),
            dma((2, 3, CHUNKS)),
            dma((2, CHUNKS)),
            dma((12, CHUNKS)),
            dma((2, CHUNKS)),
            dma((DEVICES,)),
            dma((DEVICES,)),
            dma((DEVICES,)),
            dma((DEVICES,)),
            dma((2, CHUNKS)),
        ],
        compiler_params=pltpu.CompilerParams(
            collective_id=0, has_side_effects=True, vmem_limit_bytes=67043328
        ),
        name="reduce_gradients",
    )(g_mat, g_vec_rows)


def solution(mesh):
    axis_name = mesh.axis_names[0]

    def local_step(g_mat, g_vec, p_mat, m_mat, v_mat, p_vec, m_vec, v_vec, learn_rate):
        vec_size = g_vec.shape[1]
        vec_rows = -(-vec_size // (16 * LANES)) * 16
        g_vec_rows = jnp.pad(g_vec[0], (0, vec_rows * LANES - vec_size)).reshape(vec_rows, LANES)
        grad_mat, grad_vec, clip, _ = reduce_gradients(axis_name, g_mat, g_vec_rows)
        clip_scale = clip[0, 0]
        grad_mat = grad_mat.reshape(-1)
        grad_vec = grad_vec.reshape(-1)[:vec_size]
        new_p_mat, new_m_mat, new_v_mat = adam_update(grad_mat * clip_scale, p_mat, m_mat, v_mat, learn_rate, WEIGHT_DECAY)
        new_p_vec, new_m_vec, new_v_vec = adam_update(grad_vec * clip_scale, p_vec, m_vec, v_vec, learn_rate, 0.0)
        full_params = lax.all_gather(new_p_mat.astype(jnp.bfloat16), axis_name, tiled=True)
        return new_p_mat, new_m_mat, new_v_mat, new_p_vec, new_m_vec, new_v_vec, full_params

    return jax.shard_map(
        local_step,
        mesh=mesh,
        in_specs=(P(axis_name, None), P(axis_name, None), P(axis_name), P(axis_name), P(axis_name), P(), P(), P(), P()),
        out_specs=(P(axis_name), P(axis_name), P(axis_name), P(), P(), P(), P()),
        check_vma=False,
    )
```

```python
import functools

import jax
import jax.numpy as jnp
from jax import lax
from jax.experimental import pallas as pl
from jax.experimental.pallas import tpu as pltpu
from jax.sharding import PartitionSpec as P


STEP = 10
ADAM_BETA1 = 0.9
ADAM_BETA2 = 0.98
ADAM_EPS = 1e-8
WEIGHT_DECAY = 0.01
MAX_NORM = 1.0
NORM_EPS = 1e-6
BIAS_ONE = 1.0 - ADAM_BETA1 ** STEP
BIAS_TWO = 1.0 - ADAM_BETA2 ** STEP

MESH = pl.DeviceIdType.MESH
LANES = 128
DEVICES = 8
CHUNKS = 10
BLOCK = 96
ADAM_ROWS = 480
SIZES = (1920, 7680, 7680, 1920)
NEAR_GROUPS = ((0, 1), (2,), (3,))
FAR_GROUPS = ((1, 2), (0, 3))
VMEM_ALL = 67043328


def adam_update(grad_vals, param_vals, moment_one, moment_two, learn_rate, decay_rate):
    new_one = ADAM_BETA1 * moment_one + (1.0 - ADAM_BETA1) * grad_vals
    new_two = ADAM_BETA2 * moment_two + (1.0 - ADAM_BETA2) * grad_vals * grad_vals
    direction = (new_one / BIAS_ONE) / (jnp.sqrt(new_two / BIAS_TWO) + ADAM_EPS)
    return param_vals - learn_rate * (direction + decay_rate * param_vals), new_one, new_two


def places(axis_name):
    me = lax.axis_index(axis_name)
    core, x, y = me % 2, (me // 2) % 2, me // 4

    def dev(yy, xx, cc):
        return 4 * yy + 2 * xx + cc

    return me, core, x, y, dev


def reduce_kernel(axis_name, half_rows, g_ref, gv_raw_ref, gsum_ref, vsum_ref, clip_ref, stage_ref,
                  first, own_first, direct, own_direct, fsum, psum, raw, packed, vraw, gv_ref, vrecv, nsend, nrecv,
                  vraw_sem, raw_sem, pack_sem, first_recv, direct_recv, psum_recv, send_sem, fsum_send,
                  vec_send, vec_recv, nrm_send, nrm_recv, out_sem):
    me, core, x, y, dev = places(axis_name)
    sib = dev(y, x, 1 - core)
    xs = [dev(y, 1 - x, 0), dev(y, 1 - x, 1)]
    ys = [dev(1 - y, x, 0), dev(1 - y, x, 1)]
    ds = [dev(1 - y, 1 - x, 0), dev(1 - y, 1 - x, 1)]
    x_mine, x_sib = dev(y, 1 - x, core), dev(y, 1 - x, 1 - core)
    y_mine, y_sib = dev(1 - y, x, core), dev(1 - y, x, 1 - core)
    rows = half_rows // CHUNKS
    vals = rows * LANES

    first_plan = [
        (2 * ds[0], ys[0], first, (0, core), first_recv),
        (2 * ds[0] + 1, xs[0], first, (1, core), first_recv),
        (2 * ds[1], ys[1], first, (0, core), first_recv),
        (2 * ds[1] + 1, xs[1], first, (1, core), first_recv),
        (2 * x_sib, sib, first, (0, 2), first_recv),
        (2 * y_sib + 1, sib, first, (1, 2), first_recv),
        (2 * x_mine, None, own_first, (0,), None),
        (2 * y_mine + 1, None, own_first, (1,), None),
    ]
    direct_plan = [
        (2 * ys[0], ys[0], direct, (0, core), direct_recv),
        (2 * xs[0] + 1, xs[0], direct, (1, core), direct_recv),
        (2 * ys[1], ys[1], direct, (0, core), direct_recv),
        (2 * xs[1] + 1, xs[1], direct, (1, core), direct_recv),
        (2 * sib, sib, direct, (0, 2), direct_recv),
        (2 * sib + 1, sib, direct, (1, 2), direct_recv),
        (2 * me, None, own_direct, (0,), None),
        (2 * me + 1, None, own_direct, (1,), None),
    ]

    def load_raw(plan, h, c):
        start = pl.multiple_of((plan[h][0] * CHUNKS + c) * vals, vals)
        return pltpu.make_async_copy(g_ref.at[:, pl.ds(start, vals)], raw.at[h], raw_sem.at[h])

    def stage_at(phase, h, c):
        return stage_ref.at[6 * phase + h, pl.ds(pl.multiple_of(c * rows, rows), rows), :]

    def to_stage(phase, h, c):
        return pltpu.make_async_copy(packed.at[h], stage_at(phase, h, c), pack_sem.at[h])

    def send(phase, plan, h, c):
        _, target, buf, slot, sems = plan[h]
        return pltpu.make_async_remote_copy(
            src_ref=stage_at(phase, h, c),
            dst_ref=buf.at[(*slot, pl.ds(pl.multiple_of(c * rows, rows), rows))],
            send_sem=send_sem.at[6 * phase + h, c],
            recv_sem=sems.at[(*slot, c)],
            device_id=(target,),
            device_id_type=MESH,
        )

    def pack(plan, h, c):
        _, target, buf, slot, _ = plan[h]

        def body(i, _):
            piece = raw[h, :, pl.ds(pl.multiple_of(i * BLOCK * LANES, BLOCK * LANES), BLOCK * LANES)]
            piece = piece.astype(jnp.float32).reshape(BLOCK, LANES).astype(jnp.bfloat16)
            if target is None:
                buf[(*slot, pl.ds(pl.multiple_of(c * rows + i * BLOCK, BLOCK), BLOCK), slice(None))] = piece
            else:
                packed[h, pl.ds(pl.multiple_of(i * BLOCK, BLOCK), BLOCK), :] = piece
            return 0

        lax.fori_loop(0, rows // BLOCK, body, 0)

    vec_size, vec_rows = gv_raw_ref.shape[1], gv_ref.shape[0]
    vec_load = pltpu.make_async_copy(gv_raw_ref, vraw.at[:, pl.ds(0, vec_size)], vraw_sem)
    vec_load.start()
    for h in range(8):
        load_raw(first_plan, h, 0).start()
    vraw[:, vec_size:] = jnp.zeros((1, vec_rows * LANES - vec_size), jnp.bfloat16)
    vec_load.wait()
    vec_mine = vraw[...].astype(jnp.float32).reshape(vec_rows, LANES).astype(jnp.bfloat16)
    gv_ref[...] = vec_mine
    vrecv[me] = vec_mine

    barrier = pltpu.get_barrier_semaphore()
    for o in range(1, DEVICES):
        pl.semaphore_signal(barrier, inc=1, device_id=((me + o) % DEVICES,), device_id_type=MESH)
    pl.semaphore_wait(barrier, DEVICES - 1)

    def vec_copy(o):
        return pltpu.make_async_remote_copy(
            src_ref=gv_ref, dst_ref=vrecv.at[me], send_sem=vec_send.at[o], recv_sem=vec_recv.at[me],
            device_id=((me + o) % DEVICES,), device_id_type=MESH)

    def vec_wait(o):
        src = (me + o) % DEVICES
        pltpu.make_async_copy(gv_ref, vrecv.at[src], vec_recv.at[src]).wait()

    for o in range(1, DEVICES):
        vec_copy(o).start()

    def send_phase(phase, plan, next_plan):
        def step(c, _):
            for h in range(8):
                load_raw(plan, h, c).wait()
                pack(plan, h, c)
                if next_plan is None:
                    @pl.when(c + 1 < CHUNKS)
                    def _():
                        load_raw(plan, h, c + 1).start()
                else:
                    @pl.when(c + 1 < CHUNKS)
                    def _():
                        load_raw(plan, h, c + 1).start()

                    @pl.when(c + 1 >= CHUNKS)
                    def _():
                        load_raw(next_plan, h, 0).start()
                if 1 <= h <= 6:
                    to_stage(phase, h - 1, c).start()
            for h in range(6):
                to_stage(phase, h, c).wait()
                send(phase, plan, h, c).start()
            return 0

        lax.fori_loop(0, CHUNKS, step, 0)

    send_phase(0, first_plan, direct_plan)
    send_phase(1, direct_plan, None)

    def got(buf, sems, slot, c):
        at = buf.at[(*slot, pl.ds(pl.multiple_of(c * rows, rows), rows))]
        pltpu.make_async_copy(at, at, sems.at[(*slot, c)]).wait()

    def fsum_copy(side, c):
        at = (side, pl.ds(pl.multiple_of(c * rows, rows), rows))
        return pltpu.make_async_remote_copy(
            src_ref=fsum.at[at], dst_ref=psum.at[at], send_sem=fsum_send.at[side, c], recv_sem=psum_recv.at[side, c],
            device_id=((x_mine, y_mine)[side],), device_id_type=MESH)

    def relay_step(c, _):
        for side in range(2):
            for slot in range(3):
                got(first, first_recv, (side, slot), c)

            def body(i, _, side=side):
                at = pl.ds(pl.multiple_of(c * rows + i * BLOCK, BLOCK), BLOCK)
                total = first[side, 0, at, :].astype(jnp.float32) + first[side, 1, at, :].astype(jnp.float32)
                total = total + (first[side, 2, at, :].astype(jnp.float32) + own_first[side, at, :].astype(jnp.float32))
                fsum[side, at, :] = total
                return 0

            lax.fori_loop(0, rows // BLOCK, body, 0)
            if side == 1:
                fsum_copy(0, c).start()
            else:
                @pl.when(c > 0)
                def _():
                    fsum_copy(1, c - 1).start()
        return 0

    lax.fori_loop(0, CHUNKS, relay_step, 0)

    for o in range(1, DEVICES):
        vec_wait(o)
    vec_total = vrecv[0].astype(jnp.float32)
    for d in range(1, DEVICES):
        vec_total = vec_total + vrecv[d].astype(jnp.float32)
    vec_mean = vec_total / DEVICES
    vsum_ref[...] = vec_mean
    fsum_copy(1, CHUNKS - 1).start()

    def out_copy(side, c):
        at = pl.ds(pl.multiple_of(c * rows, rows), rows)
        to = pl.ds(pl.multiple_of(side * half_rows + c * rows, rows), rows)
        return pltpu.make_async_copy(psum.at[side, at], gsum_ref.at[to], out_sem.at[side, c])

    def final_step(c, acc):
        for side in range(2):
            got(psum, psum_recv, (side,), c)
            for slot in range(3):
                got(direct, direct_recv, (side, slot), c)

            def body(i, acc, side=side):
                at = pl.ds(pl.multiple_of(c * rows + i * BLOCK, BLOCK), BLOCK)
                total = direct[side, 0, at, :].astype(jnp.float32) + direct[side, 1, at, :].astype(jnp.float32)
                total = total + (direct[side, 2, at, :].astype(jnp.float32) + own_direct[side, at, :].astype(jnp.float32))
                mean = (psum[side, at, :] + total) / DEVICES
                psum[side, at, :] = mean
                return acc + jnp.sum((mean * mean).reshape(BLOCK // 8, 8, LANES), axis=0)

            acc = lax.fori_loop(0, rows // BLOCK, body, acc)
            if side == 1:
                out_copy(0, c).start()
            else:
                @pl.when(c > 0)
                def _():
                    out_copy(1, c - 1).start()
        return acc

    acc = lax.fori_loop(0, CHUNKS, final_step, jnp.zeros((8, LANES), jnp.float32))
    nsend[...] = acc
    nrecv[me] = acc
    out_copy(1, CHUNKS - 1).start()

    def drain(c, _):
        for h in range(6):
            send(0, first_plan, h, c).wait_send()
            send(1, direct_plan, h, c).wait_send()
        return 0

    lax.fori_loop(0, CHUNKS, drain, 0)

    def nrm_copy(o):
        return pltpu.make_async_remote_copy(
            src_ref=nsend, dst_ref=nrecv.at[me], send_sem=nrm_send.at[o], recv_sem=nrm_recv.at[me],
            device_id=((me + o) % DEVICES,), device_id_type=MESH)

    def nrm_wait(o):
        src = (me + o) % DEVICES
        pltpu.make_async_copy(nsend, nrecv.at[src], nrm_recv.at[src]).wait()

    for o in range(1, DEVICES):
        nrm_copy(o).start()

    def drain_rest(c, _):
        for side in range(2):
            fsum_copy(side, c).wait_send()
            out_copy(side, c).wait()
        return 0

    lax.fori_loop(0, CHUNKS, drain_rest, 0)
    for o in range(1, DEVICES):
        vec_copy(o).wait_send()
    for o in range(1, DEVICES):
        nrm_wait(o)
    tile = jnp.sum((vec_mean * vec_mean).reshape(-1, 8, LANES), axis=0)
    for d in range(DEVICES):
        tile = tile + nrecv[d]
    norm_sq = jnp.full((8, LANES), jnp.sum(tile), jnp.float32)
    clip_ref[...] = jnp.minimum(1.0, MAX_NORM / (jnp.sqrt(norm_sq) + NORM_EPS))
    for o in range(1, DEVICES):
        nrm_copy(o).wait_send()


def reduce_gradients(axis_name, g_mat, g_vec):
    half_rows = g_mat.shape[1] // (2 * DEVICES * LANES)
    rows = half_rows // CHUNKS
    vec_rows = -(-g_vec.shape[1] // (16 * LANES)) * 16
    bf16, f32 = jnp.bfloat16, jnp.float32
    dma = pltpu.SemaphoreType.DMA
    hbm, vmem = pl.BlockSpec(memory_space=pltpu.HBM), pl.BlockSpec(memory_space=pltpu.VMEM)
    return pl.pallas_call(
        functools.partial(reduce_kernel, axis_name, half_rows),
        out_shape=(
            jax.ShapeDtypeStruct((2 * half_rows, LANES), f32),
            jax.ShapeDtypeStruct((vec_rows, LANES), f32),
            jax.ShapeDtypeStruct((8, LANES), f32),
            jax.ShapeDtypeStruct((12, half_rows, LANES), bf16),
        ),
        in_specs=[hbm, hbm],
        out_specs=(hbm, vmem, vmem, hbm),
        scratch_shapes=[
            pltpu.VMEM((2, 3, half_rows, LANES), bf16),
            pltpu.VMEM((2, half_rows, LANES), bf16),
            pltpu.VMEM((2, 3, half_rows, LANES), bf16),
            pltpu.VMEM((2, half_rows, LANES), bf16),
            pltpu.VMEM((2, half_rows, LANES), f32),
            pltpu.VMEM((2, half_rows, LANES), f32),
            pltpu.VMEM((8, 1, rows * LANES), bf16),
            pltpu.VMEM((6, rows, LANES), bf16),
            pltpu.VMEM((1, vec_rows * LANES), bf16),
            pltpu.VMEM((vec_rows, LANES), bf16),
            pltpu.VMEM((DEVICES, vec_rows, LANES), bf16),
            pltpu.VMEM((8, LANES), f32),
            pltpu.VMEM((DEVICES, 8, LANES), f32),
            dma,
            dma((8,)),
            dma((6,)),
            dma((2, 3, CHUNKS)),
            dma((2, 3, CHUNKS)),
            dma((2, CHUNKS)),
            dma((12, CHUNKS)),
            dma((2, CHUNKS)),
            dma((DEVICES,)),
            dma((DEVICES,)),
            dma((DEVICES,)),
            dma((DEVICES,)),
            dma((2, CHUNKS)),
        ],
        compiler_params=pltpu.CompilerParams(
            collective_id=0, has_side_effects=True, vmem_limit_bytes=VMEM_ALL
        ),
        name="reduce_gradients",
    )(g_mat, g_vec)


def adam_kernel(lr_ref, clip_ref, g_ref, p_ref, m_ref, v_ref, *refs):
    new_p_ref, new_m_ref, new_v_ref, narrow_ref = refs[-4:]
    grad = g_ref[...] * clip_ref[0:1, :]
    new_p, new_m, new_v = adam_update(grad, p_ref[...], m_ref[...], v_ref[...], lr_ref[0], WEIGHT_DECAY)
    new_p_ref[...] = new_p
    new_m_ref[...] = new_m
    new_v_ref[...] = new_v
    narrow_ref[...] = new_p.astype(jnp.bfloat16)


def adam_chunk(start, size, learn_rate, clip, grad, params, state):
    rows = grad.shape[0]
    here = pl.BlockSpec((ADAM_ROWS, LANES), lambda i: (start // ADAM_ROWS + i, 0))
    kept = pl.BlockSpec(memory_space=pltpu.HBM)
    whole = jax.ShapeDtypeStruct((rows, LANES), jnp.float32)
    return pl.pallas_call(
        adam_kernel,
        grid=(size // ADAM_ROWS,),
        out_shape=(whole, whole, whole, jax.ShapeDtypeStruct((size, LANES), jnp.bfloat16)),
        in_specs=[pl.BlockSpec(memory_space=pltpu.SMEM), pl.BlockSpec((8, LANES), lambda i: (0, 0)), here, here, here, here]
        + [kept] * len(state),
        out_specs=(here, here, here, pl.BlockSpec((ADAM_ROWS, LANES), lambda i: (i, 0))),
        input_output_aliases={6 + k: k for k in range(len(state))},
        cost_estimate=pl.CostEstimate(flops=size * LANES * 60, bytes_accessed=size * LANES * 30, transcendentals=0),
        compiler_params=pltpu.CompilerParams(vmem_limit_bytes=VMEM_ALL),
    )(learn_rate, clip, grad, *params, *state)


def place_kernel(axis_name, offsets, piece_rows, *refs):
    count = len(offsets)
    sources, out_ref, buffers, sems = refs[-2 * count - 3 : -count - 3], refs[-count - 3], refs[-count - 2 : -2], refs[-2:]
    _, core, x, y, dev = places(axis_name)
    owners = {"me": dev(y, x, core), "sib": dev(y, x, 1 - core),
              "x": dev(y, 1 - x, core), "x_sib": dev(y, 1 - x, 1 - core),
              "y": dev(1 - y, x, core), "y_sib": dev(1 - y, x, 1 - core),
              "d": dev(1 - y, 1 - x, core), "d_sib": dev(1 - y, 1 - x, 1 - core)}
    loads, stores = [], []
    for k, (who, start) in enumerate(offsets):
        size = sources[k].shape[0]
        at = pl.multiple_of(owners[who] * piece_rows + start, 16)
        loads.append(pltpu.make_async_copy(sources[k], buffers[k], sems[0].at[k]))
        stores.append(pltpu.make_async_copy(buffers[k], out_ref.at[pl.ds(at, size)], sems[1].at[k]))
    for load in loads:
        load.start()
    for load, store in zip(loads, stores):
        load.wait()
        store.start()
    for store in stores:
        store.wait()


def place(axis_name, piece_rows, full, items):
    hbm = pl.BlockSpec(memory_space=pltpu.HBM)
    sources = [source for _, _, source in items]
    moved = sum(source.shape[0] for source in sources)
    started = () if full is None else (full,)
    return pl.pallas_call(
        functools.partial(place_kernel, axis_name, tuple((who, start) for who, start, _ in items), piece_rows),
        out_shape=jax.ShapeDtypeStruct((DEVICES * piece_rows, LANES), jnp.bfloat16),
        in_specs=[hbm] * (len(started) + len(sources)),
        out_specs=hbm,
        input_output_aliases={0: 0} if started else {},
        scratch_shapes=[pltpu.VMEM(source.shape, jnp.bfloat16) for source in sources]
        + [pltpu.SemaphoreType.DMA((len(sources),))] * 2,
        cost_estimate=pl.CostEstimate(flops=moved * LANES * 15, bytes_accessed=moved * LANES * 4, transcendentals=0),
        compiler_params=pltpu.CompilerParams(vmem_limit_bytes=VMEM_ALL),
    )(*started, *sources)


def solution(mesh):
    axis_name = mesh.axis_names[0]
    to_sib = [(d, 4 * (d // 4) + 2 * (d // 2 % 2) + (1 - d % 2)) for d in range(DEVICES)]
    to_x = [(d, 4 * (d // 4) + 2 * (1 - d // 2 % 2) + d % 2) for d in range(DEVICES)]
    to_y = [(d, 4 * (1 - d // 4) + 2 * (d // 2 % 2) + d % 2) for d in range(DEVICES)]

    def move(array, pairs):
        return lax.ppermute(array, axis_name, pairs)

    def local_step(g_mat, g_vec, p_mat, m_mat, v_mat, p_vec, m_vec, v_vec, learn_rate):
        vec_size = g_vec.shape[1]
        grad_mat, grad_vec, clip, _ = reduce_gradients(axis_name, g_mat, g_vec)
        piece_rows = grad_mat.shape[0]
        params = [array.reshape(piece_rows, LANES) for array in (p_mat, m_mat, v_mat)]
        rate = learn_rate.reshape(1)

        state, starts, own = (), [], []
        for size in SIZES:
            starts.append(sum(SIZES[: len(starts)]))
            *state, narrow = adam_chunk(starts[-1], size, rate, clip, grad_mat, params, state)
            own.append(narrow)

        sib, from_x, from_y = [], [], []
        for chunk in own:
            from_x.append(move(chunk, to_x))
            from_y.append(move(chunk, to_y))
            sib.append(move(chunk, to_sib))
        near, far = [], []
        for j, start in enumerate(starts):
            diag = move(from_y[j], to_x) if j % 2 == 0 else move(from_x[j], to_y)
            near.append([("me", start, own[j]), ("sib", start, sib[j]),
                         ("x", start, from_x[j]), ("x_sib", start, move(from_x[j], to_sib)),
                         ("y", start, from_y[j]), ("y_sib", start, move(from_y[j], to_sib))])
            far.append([("d", start, diag), ("d_sib", start, move(diag, to_sib))])
        full = None
        for group in NEAR_GROUPS:
            full = place(axis_name, piece_rows, full, sum((near[j] for j in group), []))
        for group in FAR_GROUPS:
            full = place(axis_name, piece_rows, full, sum((far[j] for j in group), []))

        grad_vec = grad_vec.reshape(-1)[:vec_size]
        new_p_vec, new_m_vec, new_v_vec = adam_update(grad_vec * clip[0, 0], p_vec, m_vec, v_vec, learn_rate, 0.0)
        new_p, new_m, new_v = (array.reshape(-1) for array in state)
        return new_p, new_m, new_v, new_p_vec, new_m_vec, new_v_vec, full.reshape(-1)

    return jax.shard_map(
        local_step,
        mesh=mesh,
        in_specs=(P(axis_name, None), P(axis_name, None), P(axis_name), P(axis_name), P(axis_name), P(), P(), P(), P()),
        out_specs=(P(axis_name), P(axis_name), P(axis_name), P(), P(), P(), P()),
        check_vma=False,
    )
```

```python
import functools

import jax
import jax.numpy as jnp
from jax import lax
from jax.experimental import pallas as pl
from jax.experimental.pallas import tpu as pltpu
from jax.sharding import PartitionSpec as P


STEP = 10
ADAM_BETA1 = 0.9
ADAM_BETA2 = 0.98
ADAM_EPS = 1e-8
WEIGHT_DECAY = 0.01
MAX_NORM = 1.0
NORM_EPS = 1e-6
BIAS_ONE = 1.0 - ADAM_BETA1 ** STEP
BIAS_TWO = 1.0 - ADAM_BETA2 ** STEP

MESH = pl.DeviceIdType.MESH
LANES = 128
DEVICES = 8
CHUNKS = 10
BLOCK = 96
ADAM_ROWS = 480
SIZES = (1440, 2880, 5280, 5280, 2880, 1440)
NEAR_GROUPS = ((0, 1), (2,), (3,), (4, 5))
FAR_GROUPS = ((1, 2), (3, 4), (0, 5))
VMEM_ALL = 67043328


def adam_update(grad_vals, param_vals, moment_one, moment_two, learn_rate, decay_rate):
    new_one = ADAM_BETA1 * moment_one + (1.0 - ADAM_BETA1) * grad_vals
    new_two = ADAM_BETA2 * moment_two + (1.0 - ADAM_BETA2) * grad_vals * grad_vals
    direction = (new_one * (1.0 / BIAS_ONE)) / (jnp.sqrt(new_two * (1.0 / BIAS_TWO)) + ADAM_EPS)
    return param_vals - learn_rate * (direction + decay_rate * param_vals), new_one, new_two


def places(axis_name):
    me = lax.axis_index(axis_name)
    core, x, y = me % 2, (me // 2) % 2, me // 4

    def dev(yy, xx, cc):
        return 4 * yy + 2 * xx + cc

    return me, core, x, y, dev


def reduce_kernel(axis_name, half_rows, g_ref, gv_raw_ref, gsum_ref, vsum_ref, clip_ref, stage_ref,
                  first, own_first, direct, own_direct, fsum, psum, raw, packed, vraw, gv_ref, vrecv, nsend, nrecv,
                  vraw_sem, raw_sem, pack_sem, first_recv, direct_recv, psum_recv, send_sem, fsum_send,
                  vec_send, vec_recv, nrm_send, nrm_recv, out_sem):
    me, core, x, y, dev = places(axis_name)
    sib = dev(y, x, 1 - core)
    xs = [dev(y, 1 - x, 0), dev(y, 1 - x, 1)]
    ys = [dev(1 - y, x, 0), dev(1 - y, x, 1)]
    ds = [dev(1 - y, 1 - x, 0), dev(1 - y, 1 - x, 1)]
    x_mine, x_sib = dev(y, 1 - x, core), dev(y, 1 - x, 1 - core)
    y_mine, y_sib = dev(1 - y, x, core), dev(1 - y, x, 1 - core)
    rows = half_rows // CHUNKS
    vals = rows * LANES

    first_plan = [
        (2 * ds[0], ys[0], first, (0, core), first_recv),
        (2 * ds[0] + 1, xs[0], first, (1, core), first_recv),
        (2 * ds[1], ys[1], first, (0, core), first_recv),
        (2 * ds[1] + 1, xs[1], first, (1, core), first_recv),
        (2 * x_sib, sib, first, (0, 2), first_recv),
        (2 * y_sib + 1, sib, first, (1, 2), first_recv),
        (2 * x_mine, None, own_first, (0,), None),
        (2 * y_mine + 1, None, own_first, (1,), None),
    ]
    direct_plan = [
        (2 * ys[0], ys[0], direct, (0, core), direct_recv),
        (2 * xs[0] + 1, xs[0], direct, (1, core), direct_recv),
        (2 * ys[1], ys[1], direct, (0, core), direct_recv),
        (2 * xs[1] + 1, xs[1], direct, (1, core), direct_recv),
        (2 * sib, sib, direct, (0, 2), direct_recv),
        (2 * sib + 1, sib, direct, (1, 2), direct_recv),
        (2 * me, None, own_direct, (0,), None),
        (2 * me + 1, None, own_direct, (1,), None),
    ]

    def load_raw(plan, h, c):
        start = pl.multiple_of((plan[h][0] * CHUNKS + c) * vals, vals)
        return pltpu.make_async_copy(g_ref.at[:, pl.ds(start, vals)], raw.at[h], raw_sem.at[h])

    def stage_at(phase, h, c):
        return stage_ref.at[6 * phase + h, pl.ds(pl.multiple_of(c * rows, rows), rows), :]

    def to_stage(phase, h, c):
        return pltpu.make_async_copy(packed.at[h], stage_at(phase, h, c), pack_sem.at[h])

    def send(phase, plan, h, c):
        _, target, buf, slot, sems = plan[h]
        return pltpu.make_async_remote_copy(
            src_ref=stage_at(phase, h, c),
            dst_ref=buf.at[(*slot, pl.ds(pl.multiple_of(c * rows, rows), rows))],
            send_sem=send_sem.at[6 * phase + h, c],
            recv_sem=sems.at[(*slot, c)],
            device_id=(target,),
            device_id_type=MESH,
        )

    def pack(plan, h, c):
        _, target, buf, slot, _ = plan[h]

        def body(i, _):
            piece = raw[h, :, pl.ds(pl.multiple_of(i * BLOCK * LANES, BLOCK * LANES), BLOCK * LANES)]
            piece = piece.astype(jnp.float32).reshape(BLOCK, LANES).astype(jnp.bfloat16)
            if target is None:
                buf[(*slot, pl.ds(pl.multiple_of(c * rows + i * BLOCK, BLOCK), BLOCK), slice(None))] = piece
            else:
                packed[h, pl.ds(pl.multiple_of(i * BLOCK, BLOCK), BLOCK), :] = piece
            return 0

        lax.fori_loop(0, rows // BLOCK, body, 0)

    vec_size, vec_rows = gv_raw_ref.shape[1], gv_ref.shape[0]
    vec_load = pltpu.make_async_copy(gv_raw_ref, vraw.at[:, pl.ds(0, vec_size)], vraw_sem)
    vec_load.start()
    for h in range(8):
        load_raw(first_plan, h, 0).start()
    vraw[:, vec_size:] = jnp.zeros((1, vec_rows * LANES - vec_size), jnp.bfloat16)
    vec_load.wait()
    vec_mine = vraw[...].astype(jnp.float32).reshape(vec_rows, LANES).astype(jnp.bfloat16)
    gv_ref[...] = vec_mine
    vrecv[me] = vec_mine

    def pack_all(phase, plan, next_plan, c):
        for h in range(8):
            load_raw(plan, h, c).wait()
            pack(plan, h, c)

            @pl.when(c + 1 < CHUNKS)
            def _():
                load_raw(plan, h, c + 1).start()

            if next_plan is not None:
                @pl.when(c + 1 >= CHUNKS)
                def _():
                    load_raw(next_plan, h, 0).start()

            if 1 <= h <= 6:
                to_stage(phase, h - 1, c).start()

    def send_all(phase, plan, c):
        for h in range(6):
            to_stage(phase, h, c).wait()
            send(phase, plan, h, c).start()

    def step(phase, plan, next_plan):
        def body(c, _):
            pack_all(phase, plan, next_plan, c)
            send_all(phase, plan, c)
            return 0

        return body

    pack_all(0, first_plan, direct_plan, 0)

    barrier = pltpu.get_barrier_semaphore()
    for o in range(1, DEVICES):
        pl.semaphore_signal(barrier, inc=1, device_id=((me + o) % DEVICES,), device_id_type=MESH)
    pl.semaphore_wait(barrier, DEVICES - 1)

    def vec_copy(o):
        return pltpu.make_async_remote_copy(
            src_ref=gv_ref, dst_ref=vrecv.at[me], send_sem=vec_send.at[o], recv_sem=vec_recv.at[me],
            device_id=((me + o) % DEVICES,), device_id_type=MESH)

    def vec_wait(o):
        src = (me + o) % DEVICES
        pltpu.make_async_copy(gv_ref, vrecv.at[src], vec_recv.at[src]).wait()

    for o in range(1, DEVICES):
        vec_copy(o).start()

    send_all(0, first_plan, 0)
    lax.fori_loop(1, CHUNKS, step(0, first_plan, direct_plan), 0)
    lax.fori_loop(0, CHUNKS, step(1, direct_plan, None), 0)

    def got(buf, sems, slot, c):
        at = buf.at[(*slot, pl.ds(pl.multiple_of(c * rows, rows), rows))]
        pltpu.make_async_copy(at, at, sems.at[(*slot, c)]).wait()

    def fsum_copy(side, c):
        at = (side, pl.ds(pl.multiple_of(c * rows, rows), rows))
        return pltpu.make_async_remote_copy(
            src_ref=fsum.at[at], dst_ref=psum.at[at], send_sem=fsum_send.at[side, c], recv_sem=psum_recv.at[side, c],
            device_id=((x_mine, y_mine)[side],), device_id_type=MESH)

    def relay_step(c, _):
        for side in range(2):
            for slot in range(3):
                got(first, first_recv, (side, slot), c)

            def body(i, _, side=side):
                at = pl.ds(pl.multiple_of(c * rows + i * BLOCK, BLOCK), BLOCK)
                total = first[side, 0, at, :].astype(jnp.float32) + first[side, 1, at, :].astype(jnp.float32)
                total = total + (first[side, 2, at, :].astype(jnp.float32) + own_first[side, at, :].astype(jnp.float32))
                fsum[side, at, :] = total
                return 0

            lax.fori_loop(0, rows // BLOCK, body, 0)
            if side == 1:
                fsum_copy(0, c).start()
            else:
                @pl.when(c > 0)
                def _():
                    fsum_copy(1, c - 1).start()
        return 0

    lax.fori_loop(0, CHUNKS, relay_step, 0)

    for o in range(1, DEVICES):
        vec_wait(o)
    vec_total = vrecv[0].astype(jnp.float32)
    for d in range(1, DEVICES):
        vec_total = vec_total + vrecv[d].astype(jnp.float32)
    vec_mean = vec_total / DEVICES
    vsum_ref[...] = vec_mean
    fsum_copy(1, CHUNKS - 1).start()

    def out_copy(side, c):
        at = pl.ds(pl.multiple_of(c * rows, rows), rows)
        to = pl.ds(pl.multiple_of(side * half_rows + c * rows, rows), rows)
        return pltpu.make_async_copy(psum.at[side, at], gsum_ref.at[to], out_sem.at[side, c])

    def final_step(c, acc):
        for side in range(2):
            got(psum, psum_recv, (side,), c)
            for slot in range(3):
                got(direct, direct_recv, (side, slot), c)

            def body(i, acc, side=side):
                at = pl.ds(pl.multiple_of(c * rows + i * BLOCK, BLOCK), BLOCK)
                total = direct[side, 0, at, :].astype(jnp.float32) + direct[side, 1, at, :].astype(jnp.float32)
                total = total + (direct[side, 2, at, :].astype(jnp.float32) + own_direct[side, at, :].astype(jnp.float32))
                mean = (psum[side, at, :] + total) / DEVICES
                psum[side, at, :] = mean
                return acc + jnp.sum((mean * mean).reshape(BLOCK // 8, 8, LANES), axis=0)

            acc = lax.fori_loop(0, rows // BLOCK, body, acc)
            if side == 1:
                out_copy(0, c).start()
            else:
                @pl.when(c > 0)
                def _():
                    out_copy(1, c - 1).start()
        return acc

    acc = lax.fori_loop(0, CHUNKS, final_step, jnp.zeros((8, LANES), jnp.float32))
    nsend[...] = acc
    nrecv[me] = acc
    out_copy(1, CHUNKS - 1).start()

    def drain(c, _):
        for h in range(6):
            send(0, first_plan, h, c).wait_send()
            send(1, direct_plan, h, c).wait_send()
        return 0

    lax.fori_loop(0, CHUNKS, drain, 0)

    def nrm_copy(o):
        return pltpu.make_async_remote_copy(
            src_ref=nsend, dst_ref=nrecv.at[me], send_sem=nrm_send.at[o], recv_sem=nrm_recv.at[me],
            device_id=((me + o) % DEVICES,), device_id_type=MESH)

    def nrm_wait(o):
        src = (me + o) % DEVICES
        pltpu.make_async_copy(nsend, nrecv.at[src], nrm_recv.at[src]).wait()

    for o in range(1, DEVICES):
        nrm_copy(o).start()

    def drain_rest(c, _):
        for side in range(2):
            fsum_copy(side, c).wait_send()
            out_copy(side, c).wait()
        return 0

    lax.fori_loop(0, CHUNKS, drain_rest, 0)
    for o in range(1, DEVICES):
        vec_copy(o).wait_send()
    for o in range(1, DEVICES):
        nrm_wait(o)
    tile = jnp.sum((vec_mean * vec_mean).reshape(-1, 8, LANES), axis=0)
    for d in range(DEVICES):
        tile = tile + nrecv[d]
    norm_sq = jnp.full((8, LANES), jnp.sum(tile), jnp.float32)
    clip_ref[...] = jnp.minimum(1.0, MAX_NORM / (jnp.sqrt(norm_sq) + NORM_EPS))
    for o in range(1, DEVICES):
        nrm_copy(o).wait_send()


def reduce_gradients(axis_name, g_mat, g_vec):
    half_rows = g_mat.shape[1] // (2 * DEVICES * LANES)
    rows = half_rows // CHUNKS
    vec_rows = -(-g_vec.shape[1] // (16 * LANES)) * 16
    bf16, f32 = jnp.bfloat16, jnp.float32
    dma = pltpu.SemaphoreType.DMA
    hbm, vmem = pl.BlockSpec(memory_space=pltpu.HBM), pl.BlockSpec(memory_space=pltpu.VMEM)
    return pl.pallas_call(
        functools.partial(reduce_kernel, axis_name, half_rows),
        out_shape=(
            jax.ShapeDtypeStruct((2 * half_rows, LANES), f32),
            jax.ShapeDtypeStruct((vec_rows, LANES), f32),
            jax.ShapeDtypeStruct((8, LANES), f32),
            jax.ShapeDtypeStruct((12, half_rows, LANES), bf16),
        ),
        in_specs=[hbm, hbm],
        out_specs=(hbm, vmem, vmem, hbm),
        scratch_shapes=[
            pltpu.VMEM((2, 3, half_rows, LANES), bf16),
            pltpu.VMEM((2, half_rows, LANES), bf16),
            pltpu.VMEM((2, 3, half_rows, LANES), bf16),
            pltpu.VMEM((2, half_rows, LANES), bf16),
            pltpu.VMEM((2, half_rows, LANES), f32),
            pltpu.VMEM((2, half_rows, LANES), f32),
            pltpu.VMEM((8, 1, rows * LANES), bf16),
            pltpu.VMEM((6, rows, LANES), bf16),
            pltpu.VMEM((1, vec_rows * LANES), bf16),
            pltpu.VMEM((vec_rows, LANES), bf16),
            pltpu.VMEM((DEVICES, vec_rows, LANES), bf16),
            pltpu.VMEM((8, LANES), f32),
            pltpu.VMEM((DEVICES, 8, LANES), f32),
            dma,
            dma((8,)),
            dma((6,)),
            dma((2, 3, CHUNKS)),
            dma((2, 3, CHUNKS)),
            dma((2, CHUNKS)),
            dma((12, CHUNKS)),
            dma((2, CHUNKS)),
            dma((DEVICES,)),
            dma((DEVICES,)),
            dma((DEVICES,)),
            dma((DEVICES,)),
            dma((2, CHUNKS)),
        ],
        compiler_params=pltpu.CompilerParams(
            collective_id=0, has_side_effects=True, vmem_limit_bytes=VMEM_ALL
        ),
        name="reduce_gradients",
    )(g_mat, g_vec)


def adam_kernel(start, lr_ref, clip_ref, *refs):
    inputs, outputs, (wide, narrow, load_sem, store_sem) = refs[:4], refs[-8:-4], refs[-4:]
    count = narrow.shape[0] // ADAM_ROWS

    def rows(i, base=0):
        return pl.ds(pl.multiple_of(base + i * ADAM_ROWS, ADAM_ROWS), ADAM_ROWS)

    def load(k, i):
        return pltpu.make_async_copy(inputs[k].at[rows(i, start)], wide.at[k, rows(i)], load_sem.at[k, i])

    def store(k, i):
        if k == 3:
            return pltpu.make_async_copy(narrow.at[rows(i)], outputs[3].at[rows(i)], store_sem.at[3, i])
        return pltpu.make_async_copy(wide.at[k + 1, rows(i)], outputs[k].at[rows(i, start)], store_sem.at[k, i])

    for i in range(count):
        for k in range(4):
            load(k, i).start()

    def step(i, _):
        for k in range(4):
            load(k, i).wait()
        at = rows(i)
        grad = wide[0, at, :] * clip_ref[0:1, :]
        new_p, new_m, new_v = adam_update(grad, wide[1, at, :], wide[2, at, :], wide[3, at, :], lr_ref[0], WEIGHT_DECAY)
        wide[1, at, :] = new_p
        wide[2, at, :] = new_m
        wide[3, at, :] = new_v
        narrow[at, :] = new_p.astype(jnp.bfloat16)

        @pl.when(i > 0)
        def _():
            for k in (3, 0, 1, 2):
                store(k, i - 1).start()

        return 0

    lax.fori_loop(0, count, step, 0)
    for k in (3, 0, 1, 2):
        store(k, count - 1).start()
    for i in range(count):
        for k in range(4):
            store(k, i).wait()


def adam_chunk(start, size, learn_rate, clip, grad, params, state):
    hbm = pl.BlockSpec(memory_space=pltpu.HBM)
    whole = jax.ShapeDtypeStruct(grad.shape, jnp.float32)
    return pl.pallas_call(
        functools.partial(adam_kernel, start),
        out_shape=(whole, whole, whole, jax.ShapeDtypeStruct((size, LANES), jnp.bfloat16)),
        in_specs=[pl.BlockSpec(memory_space=pltpu.SMEM), pl.BlockSpec(memory_space=pltpu.VMEM)] + [hbm] * (4 + len(state)),
        out_specs=(hbm, hbm, hbm, hbm),
        input_output_aliases={6 + k: k for k in range(len(state))},
        scratch_shapes=[
            pltpu.VMEM((4, size, LANES), jnp.float32),
            pltpu.VMEM((size, LANES), jnp.bfloat16),
            pltpu.SemaphoreType.DMA((4, size // ADAM_ROWS)),
            pltpu.SemaphoreType.DMA((4, size // ADAM_ROWS)),
        ],
        cost_estimate=pl.CostEstimate(flops=size * LANES * 60, bytes_accessed=size * LANES * 30, transcendentals=0),
        compiler_params=pltpu.CompilerParams(vmem_limit_bytes=VMEM_ALL),
    )(learn_rate, clip, grad, *params, *state)


def place_kernel(axis_name, offsets, piece_rows, *refs):
    count = len(offsets)
    sources, out_ref, buffers, sems = refs[-2 * count - 3 : -count - 3], refs[-count - 3], refs[-count - 2 : -2], refs[-2:]
    _, core, x, y, dev = places(axis_name)
    owners = {"me": dev(y, x, core), "sib": dev(y, x, 1 - core),
              "x": dev(y, 1 - x, core), "x_sib": dev(y, 1 - x, 1 - core),
              "y": dev(1 - y, x, core), "y_sib": dev(1 - y, x, 1 - core),
              "d": dev(1 - y, 1 - x, core), "d_sib": dev(1 - y, 1 - x, 1 - core)}
    loads, stores = [], []
    for k, (who, start) in enumerate(offsets):
        size = sources[k].shape[0]
        at = pl.multiple_of(owners[who] * piece_rows + start, 16)
        loads.append(pltpu.make_async_copy(sources[k], buffers[k], sems[0].at[k]))
        stores.append(pltpu.make_async_copy(buffers[k], out_ref.at[pl.ds(at, size)], sems[1].at[k]))
    for load in loads:
        load.start()
    for load, store in zip(loads, stores):
        load.wait()
        store.start()
    for store in stores:
        store.wait()


def place(axis_name, piece_rows, full, items):
    hbm = pl.BlockSpec(memory_space=pltpu.HBM)
    sources = [source for _, _, source in items]
    moved = sum(source.shape[0] for source in sources)
    started = () if full is None else (full,)
    return pl.pallas_call(
        functools.partial(place_kernel, axis_name, tuple((who, start) for who, start, _ in items), piece_rows),
        out_shape=jax.ShapeDtypeStruct((DEVICES * piece_rows, LANES), jnp.bfloat16),
        in_specs=[hbm] * (len(started) + len(sources)),
        out_specs=hbm,
        input_output_aliases={0: 0} if started else {},
        scratch_shapes=[pltpu.VMEM(source.shape, jnp.bfloat16) for source in sources]
        + [pltpu.SemaphoreType.DMA((len(sources),))] * 2,
        cost_estimate=pl.CostEstimate(flops=moved * LANES * 15, bytes_accessed=moved * LANES * 4, transcendentals=0),
        compiler_params=pltpu.CompilerParams(vmem_limit_bytes=VMEM_ALL),
    )(*started, *sources)


def solution(mesh):
    axis_name = mesh.axis_names[0]
    to_sib = [(d, 4 * (d // 4) + 2 * (d // 2 % 2) + (1 - d % 2)) for d in range(DEVICES)]
    to_x = [(d, 4 * (d // 4) + 2 * (1 - d // 2 % 2) + d % 2) for d in range(DEVICES)]
    to_y = [(d, 4 * (1 - d // 4) + 2 * (d // 2 % 2) + d % 2) for d in range(DEVICES)]

    def move(array, pairs):
        return lax.ppermute(array, axis_name, pairs)

    def local_step(g_mat, g_vec, p_mat, m_mat, v_mat, p_vec, m_vec, v_vec, learn_rate):
        vec_size = g_vec.shape[1]
        grad_mat, grad_vec, clip, _ = reduce_gradients(axis_name, g_mat, g_vec)
        piece_rows = grad_mat.shape[0]
        params = [array.reshape(piece_rows, LANES) for array in (p_mat, m_mat, v_mat)]
        rate = learn_rate.reshape(1)

        state, starts, own = (), [], []
        for size in SIZES:
            starts.append(sum(SIZES[: len(starts)]))
            *state, narrow = adam_chunk(starts[-1], size, rate, clip, grad_mat, params, state)
            own.append(narrow)

        sib, from_x, from_y = [], [], []
        for chunk in own:
            from_x.append(move(chunk, to_x))
            from_y.append(move(chunk, to_y))
            sib.append(move(chunk, to_sib))
        near, far = [], []
        for j, start in enumerate(starts):
            diag = move(from_y[j], to_x) if j % 2 == 0 else move(from_x[j], to_y)
            near.append([("me", start, own[j]), ("sib", start, sib[j]),
                         ("x", start, from_x[j]), ("x_sib", start, move(from_x[j], to_sib)),
                         ("y", start, from_y[j]), ("y_sib", start, move(from_y[j], to_sib))])
            far.append([("d", start, diag), ("d_sib", start, move(diag, to_sib))])
        full = None
        for group in NEAR_GROUPS:
            full = place(axis_name, piece_rows, full, sum((near[j] for j in group), []))
        for group in FAR_GROUPS:
            full = place(axis_name, piece_rows, full, sum((far[j] for j in group), []))

        grad_vec = grad_vec.reshape(-1)[:vec_size]
        new_p_vec, new_m_vec, new_v_vec = adam_update(grad_vec * clip[0, 0], p_vec, m_vec, v_vec, learn_rate, 0.0)
        new_p, new_m, new_v = (array.reshape(-1) for array in state)
        return new_p, new_m, new_v, new_p_vec, new_m_vec, new_v_vec, full.reshape(-1)

    return jax.shard_map(
        local_step,
        mesh=mesh,
        in_specs=(P(axis_name, None), P(axis_name, None), P(axis_name), P(axis_name), P(axis_name), P(), P(), P(), P()),
        out_specs=(P(axis_name), P(axis_name), P(axis_name), P(), P(), P(), P()),
        check_vma=False,
    )
```

```python
import functools

import jax
import jax.numpy as jnp
from jax import lax
from jax.experimental import pallas as pl
from jax.experimental.pallas import tpu as pltpu
from jax.sharding import PartitionSpec as P


STEP = 10
ADAM_BETA1 = 0.9
ADAM_BETA2 = 0.98
ADAM_EPS = 1e-8
WEIGHT_DECAY = 0.01
MAX_NORM = 1.0
NORM_EPS = 1e-6
BIAS_ONE = 1.0 - ADAM_BETA1 ** STEP
BIAS_TWO = 1.0 - ADAM_BETA2 ** STEP

MESH = pl.DeviceIdType.MESH
LANES = 128
DEVICES = 8
CHUNKS = 12
BLOCK = 160
ADAM_ROWS = 480
HEAD_ROWS = 480
SIZES = (1440, 2400, 5280, 5760, 2880, 1440)
NEAR_GROUPS = ((0, 1), (2,), (3,), (4, 5))
FAR_GROUPS = ((1, 2), (3, 4), (0, 5))
VMEM_ALL = 67043328


def adam_update(grad_vals, param_vals, moment_one, moment_two, learn_rate, decay_rate):
    new_one = ADAM_BETA1 * moment_one + (1.0 - ADAM_BETA1) * grad_vals
    new_two = ADAM_BETA2 * moment_two + (1.0 - ADAM_BETA2) * grad_vals * grad_vals
    direction = (new_one * (1.0 / BIAS_ONE)) / (jnp.sqrt(new_two * (1.0 / BIAS_TWO)) + ADAM_EPS)
    return param_vals - learn_rate * (direction + decay_rate * param_vals), new_one, new_two


def places(axis_name):
    me = lax.axis_index(axis_name)
    core, x, y = me % 2, (me // 2) % 2, me // 4

    def dev(yy, xx, cc):
        return 4 * yy + 2 * xx + cc

    return me, core, x, y, dev


def reduce_kernel(axis_name, half_rows, lr_ref, g_ref, gv_raw_ref, p_ref, m_ref, v_ref,
                  gsum_ref, vsum_ref, clip_ref, head_ref, stage_ref,
                  first, own_first, direct, own_direct, fsum, psum, raw, packed, vraw, vsend, vrecv, vpart, vall, nsend, nrecv,
                  clip, head_state, head,
                  vraw_sem, raw_sem, pack_sem, first_recv, direct_recv, psum_recv, send_sem, fsum_send,
                  vec_send, vec_recv, part_send, part_recv, nrm_send, nrm_recv, out_sem,
                  late_sem, head_sem):
    me, core, x, y, dev = places(axis_name)
    barrier = pltpu.get_barrier_semaphore()
    for o in range(1, DEVICES):
        pl.semaphore_signal(barrier, inc=1, device_id=((me + o) % DEVICES,), device_id_type=MESH)
    sib = dev(y, x, 1 - core)
    xs = [dev(y, 1 - x, 0), dev(y, 1 - x, 1)]
    ys = [dev(1 - y, x, 0), dev(1 - y, x, 1)]
    ds = [dev(1 - y, 1 - x, 0), dev(1 - y, 1 - x, 1)]
    x_mine, x_sib = dev(y, 1 - x, core), dev(y, 1 - x, 1 - core)
    y_mine, y_sib = dev(1 - y, x, core), dev(1 - y, x, 1 - core)
    rows = half_rows // CHUNKS
    vals = rows * LANES

    first_plan = [
        (2 * ds[0], ys[0], first, (0, core), first_recv),
        (2 * ds[0] + 1, xs[0], first, (1, core), first_recv),
        (2 * ds[1], ys[1], first, (0, core), first_recv),
        (2 * ds[1] + 1, xs[1], first, (1, core), first_recv),
        (2 * x_sib, sib, first, (0, 2), first_recv),
        (2 * y_sib + 1, sib, first, (1, 2), first_recv),
        (2 * x_mine, None, own_first, (0,), None),
        (2 * y_mine + 1, None, own_first, (1,), None),
    ]
    direct_plan = [
        (2 * ys[0], ys[0], direct, (0, core), direct_recv),
        (2 * xs[0] + 1, xs[0], direct, (1, core), direct_recv),
        (2 * ys[1], ys[1], direct, (0, core), direct_recv),
        (2 * xs[1] + 1, xs[1], direct, (1, core), direct_recv),
        (2 * sib, sib, direct, (0, 2), direct_recv),
        (2 * sib + 1, sib, direct, (1, 2), direct_recv),
        (2 * me, None, own_direct, (0,), None),
        (2 * me + 1, None, own_direct, (1,), None),
    ]

    def load_raw(plan, h, c):
        start = pl.multiple_of((plan[h][0] * CHUNKS + c) * vals, vals)
        return pltpu.make_async_copy(g_ref.at[:, pl.ds(start, vals)], raw.at[h], raw_sem.at[h])

    def stage_at(phase, h, c):
        return stage_ref.at[6 * phase + h, pl.ds(pl.multiple_of(c * rows, rows), rows), :]

    def to_stage(phase, h, c):
        return pltpu.make_async_copy(packed.at[h], stage_at(phase, h, c), pack_sem.at[h])

    def send(phase, plan, h, c):
        _, target, buf, slot, sems = plan[h]
        return pltpu.make_async_remote_copy(
            src_ref=stage_at(phase, h, c),
            dst_ref=buf.at[(*slot, pl.ds(pl.multiple_of(c * rows, rows), rows))],
            send_sem=send_sem.at[6 * phase + h, c],
            recv_sem=sems.at[(*slot, c)],
            device_id=(target,),
            device_id_type=MESH,
        )

    def pack(plan, h, c):
        _, target, buf, slot, _ = plan[h]

        def body(i, _):
            piece = raw[h, :, pl.ds(pl.multiple_of(i * BLOCK * LANES, BLOCK * LANES), BLOCK * LANES)]
            piece = piece.astype(jnp.float32).reshape(BLOCK, LANES).astype(jnp.bfloat16)
            if target is None:
                buf[(*slot, pl.ds(pl.multiple_of(c * rows + i * BLOCK, BLOCK), BLOCK), slice(None))] = piece
            else:
                packed[h, pl.ds(pl.multiple_of(i * BLOCK, BLOCK), BLOCK), :] = piece
            return 0

        lax.fori_loop(0, rows // BLOCK, body, 0)

    vec_size, vec_rows = gv_raw_ref.shape[1], vsend.shape[1]
    vec_load = pltpu.make_async_copy(gv_raw_ref, vraw.at[:, pl.ds(0, vec_size)], vraw_sem)
    vec_load.start()
    for h in range(8):
        load_raw(first_plan, h, 0).start()
    vraw[:, vec_size:] = jnp.zeros((1, vraw.shape[1] - vec_size), jnp.bfloat16)
    vec_load.wait()
    vsend[...] = vraw[...].astype(jnp.float32).reshape(DEVICES, vec_rows, LANES).astype(jnp.bfloat16)
    vrecv[me] = vsend[me]

    def pack_all(phase, plan, next_plan, c):
        for h in range(8):
            load_raw(plan, h, c).wait()
            pack(plan, h, c)

            @pl.when(c + 1 < CHUNKS)
            def _():
                load_raw(plan, h, c + 1).start()

            if next_plan is not None:
                @pl.when(c + 1 >= CHUNKS)
                def _():
                    load_raw(next_plan, h, 0).start()

            if 1 <= h <= 6:
                to_stage(phase, h - 1, c).start()

    def send_all(phase, plan, c):
        for h in range(6):
            to_stage(phase, h, c).wait()
            send(phase, plan, h, c).start()

    def step(phase, plan, next_plan):
        def body(c, _):
            pack_all(phase, plan, next_plan, c)
            send_all(phase, plan, c)
            return 0

        return body

    pack_all(0, first_plan, direct_plan, 0)

    pl.semaphore_wait(barrier, DEVICES - 1)

    def vec_copy(o):
        target = (me + o) % DEVICES
        return pltpu.make_async_remote_copy(
            src_ref=vsend.at[target], dst_ref=vrecv.at[me], send_sem=vec_send.at[o], recv_sem=vec_recv.at[me],
            device_id=(target,), device_id_type=MESH)

    def part_copy(o):
        return pltpu.make_async_remote_copy(
            src_ref=vpart, dst_ref=vall.at[me], send_sem=part_send.at[o], recv_sem=part_recv.at[me],
            device_id=((me + o) % DEVICES,), device_id_type=MESH)

    def landed(buf, sems, o):
        src = (me + o) % DEVICES
        pltpu.make_async_copy(buf.at[src], buf.at[src], sems.at[src]).wait()

    for o in range(1, DEVICES):
        vec_copy(o).start()

    send_all(0, first_plan, 0)
    lax.fori_loop(1, CHUNKS, step(0, first_plan, direct_plan), 0)
    for o in range(1, DEVICES):
        landed(vrecv, vec_recv, o)
    vec_total = vrecv[0].astype(jnp.float32)
    for d in range(1, DEVICES):
        vec_total = vec_total + vrecv[d].astype(jnp.float32)
    vpart[...] = vec_total / DEVICES
    vall[me] = vec_total / DEVICES
    lax.fori_loop(0, CHUNKS, step(1, direct_plan, None), 0)
    for o in range(1, DEVICES):
        part_copy(o).start()

    def got(buf, sems, slot, c):
        at = buf.at[(*slot, pl.ds(pl.multiple_of(c * rows, rows), rows))]
        pltpu.make_async_copy(at, at, sems.at[(*slot, c)]).wait()

    def fsum_copy(side, c):
        at = (side, pl.ds(pl.multiple_of(c * rows, rows), rows))
        return pltpu.make_async_remote_copy(
            src_ref=fsum.at[at], dst_ref=psum.at[at], send_sem=fsum_send.at[side, c], recv_sem=psum_recv.at[side, c],
            device_id=((x_mine, y_mine)[side],), device_id_type=MESH)

    def relay_step(c, _):
        for side in range(2):
            for slot in range(3):
                got(first, first_recv, (side, slot), c)

            def body(i, _, side=side):
                at = pl.ds(pl.multiple_of(c * rows + i * BLOCK, BLOCK), BLOCK)
                total = first[side, 0, at, :].astype(jnp.float32) + first[side, 1, at, :].astype(jnp.float32)
                total = total + (first[side, 2, at, :].astype(jnp.float32) + own_first[side, at, :].astype(jnp.float32))
                fsum[side, at, :] = total
                return 0

            lax.fori_loop(0, rows // BLOCK, body, 0)
            if side == 1:
                fsum_copy(0, c).start()
            else:
                @pl.when(c > 0)
                def _():
                    fsum_copy(1, c - 1).start()
        return 0

    lax.fori_loop(0, CHUNKS, relay_step, 0)

    fsum_copy(1, CHUNKS - 1).start()
    for o in range(1, DEVICES):
        landed(vall, part_recv, o)
    vec_norm = jnp.sum((vall[...] * vall[...]).reshape(-1, 8, LANES), axis=0)
    vec_out = pltpu.make_async_copy(vall, vsum_ref, late_sem.at[0])
    vec_out.start()
    head_rows = head.shape[0]
    head_loads = [pltpu.make_async_copy(ref.at[pl.ds(0, head_rows)], head_state.at[k], head_sem.at[k])
                  for k, ref in enumerate((p_ref, m_ref, v_ref))]
    for load in head_loads:
        load.start()

    def out_copy(side, c):
        at = pl.ds(pl.multiple_of(c * rows, rows), rows)
        to = pl.ds(pl.multiple_of(side * half_rows + c * rows, rows), rows)
        return pltpu.make_async_copy(psum.at[side, at], gsum_ref.at[to], out_sem.at[side, c])

    def final_step(c, acc):
        for side in range(2):
            got(psum, psum_recv, (side,), c)
            for slot in range(3):
                got(direct, direct_recv, (side, slot), c)

            def body(i, acc, side=side):
                at = pl.ds(pl.multiple_of(c * rows + i * BLOCK, BLOCK), BLOCK)
                total = direct[side, 0, at, :].astype(jnp.float32) + direct[side, 1, at, :].astype(jnp.float32)
                total = total + (direct[side, 2, at, :].astype(jnp.float32) + own_direct[side, at, :].astype(jnp.float32))
                mean = (psum[side, at, :] + total) / DEVICES
                psum[side, at, :] = mean
                return acc + jnp.sum((mean * mean).reshape(BLOCK // 8, 8, LANES), axis=0)

            acc = lax.fori_loop(0, rows // BLOCK, body, acc)
            if side == 1:
                out_copy(0, c).start()
            else:
                @pl.when(c > 0)
                def _():
                    out_copy(1, c - 1).start()
        return acc

    acc = lax.fori_loop(0, CHUNKS, final_step, jnp.zeros((8, LANES), jnp.float32))
    nsend[...] = acc
    nrecv[me] = acc
    out_copy(1, CHUNKS - 1).start()

    def drain(c, _):
        for h in range(6):
            send(0, first_plan, h, c).wait_send()
            send(1, direct_plan, h, c).wait_send()
        return 0

    lax.fori_loop(0, CHUNKS, drain, 0)

    def nrm_copy(o):
        return pltpu.make_async_remote_copy(
            src_ref=nsend, dst_ref=nrecv.at[me], send_sem=nrm_send.at[o], recv_sem=nrm_recv.at[me],
            device_id=((me + o) % DEVICES,), device_id_type=MESH)

    for o in range(1, DEVICES):
        nrm_copy(o).start()

    def drain_rest(c, _):
        for side in range(2):
            fsum_copy(side, c).wait_send()
            out_copy(side, c).wait()
        return 0

    lax.fori_loop(0, CHUNKS, drain_rest, 0)
    for o in range(1, DEVICES):
        vec_copy(o).wait_send()
        part_copy(o).wait_send()
    for o in range(1, DEVICES):
        landed(nrecv, nrm_recv, o)
    tile = vec_norm
    for d in range(DEVICES):
        tile = tile + nrecv[d]
    norm_sq = jnp.full((8, LANES), jnp.sum(tile), jnp.float32)
    clip_tile = jnp.minimum(1.0, MAX_NORM / (jnp.sqrt(norm_sq) + NORM_EPS))
    clip[...] = clip_tile

    def head_copy(i):
        at = pl.ds(i * HEAD_ROWS, HEAD_ROWS)
        return pltpu.make_async_copy(head.at[at], head_ref.at[at], head_sem.at[3 + i])

    for load in head_loads:
        load.wait()
    clip_out = pltpu.make_async_copy(clip, clip_ref, late_sem.at[1])
    count = head_rows // HEAD_ROWS
    for i in range(count):
        at = pl.ds(i * HEAD_ROWS, HEAD_ROWS)
        new_p, _, _ = adam_update(psum[0, at, :] * clip_tile[0:1, :], head_state[0, at, :], head_state[1, at, :],
                                  head_state[2, at, :], lr_ref[0], WEIGHT_DECAY)
        head[at, :] = new_p.astype(jnp.bfloat16)
        if i == 0:
            clip_out.start()
        else:
            head_copy(i - 1).start()
    for o in range(1, DEVICES):
        nrm_copy(o).wait_send()
    vec_out.wait()
    head_copy(count - 1).start()
    clip_out.wait()
    for i in range(count):
        head_copy(i).wait()


def reduce_gradients(axis_name, learn_rate, g_mat, g_vec, params):
    half_rows = g_mat.shape[1] // (2 * DEVICES * LANES)
    rows = half_rows // CHUNKS
    vec_rows = -(-g_vec.shape[1] // (8 * LANES * DEVICES)) * 8
    bf16, f32 = jnp.bfloat16, jnp.float32
    dma = pltpu.SemaphoreType.DMA
    hbm = pl.BlockSpec(memory_space=pltpu.HBM)
    return pl.pallas_call(
        functools.partial(reduce_kernel, axis_name, half_rows),
        out_shape=(
            jax.ShapeDtypeStruct((2 * half_rows, LANES), f32),
            jax.ShapeDtypeStruct((DEVICES, vec_rows, LANES), f32),
            jax.ShapeDtypeStruct((8, LANES), f32),
            jax.ShapeDtypeStruct((SIZES[0], LANES), bf16),
            jax.ShapeDtypeStruct((12, half_rows, LANES), bf16),
        ),
        in_specs=[pl.BlockSpec(memory_space=pltpu.SMEM)] + [hbm] * 5,
        out_specs=(hbm,) * 5,
        scratch_shapes=[
            pltpu.VMEM((2, 3, half_rows, LANES), bf16),
            pltpu.VMEM((2, half_rows, LANES), bf16),
            pltpu.VMEM((2, 3, half_rows, LANES), bf16),
            pltpu.VMEM((2, half_rows, LANES), bf16),
            pltpu.VMEM((2, half_rows, LANES), f32),
            pltpu.VMEM((2, half_rows, LANES), f32),
            pltpu.VMEM((8, 1, rows * LANES), bf16),
            pltpu.VMEM((6, rows, LANES), bf16),
            pltpu.VMEM((1, DEVICES * vec_rows * LANES), bf16),
            pltpu.VMEM((DEVICES, vec_rows, LANES), bf16),
            pltpu.VMEM((DEVICES, vec_rows, LANES), bf16),
            pltpu.VMEM((vec_rows, LANES), f32),
            pltpu.VMEM((DEVICES, vec_rows, LANES), f32),
            pltpu.VMEM((8, LANES), f32),
            pltpu.VMEM((DEVICES, 8, LANES), f32),
            pltpu.VMEM((8, LANES), f32),
            pltpu.VMEM((3, SIZES[0], LANES), f32),
            pltpu.VMEM((SIZES[0], LANES), bf16),
            dma,
            dma((8,)),
            dma((6,)),
            dma((2, 3, CHUNKS)),
            dma((2, 3, CHUNKS)),
            dma((2, CHUNKS)),
            dma((12, CHUNKS)),
            dma((2, CHUNKS)),
            dma((DEVICES,)),
            dma((DEVICES,)),
            dma((DEVICES,)),
            dma((DEVICES,)),
            dma((DEVICES,)),
            dma((DEVICES,)),
            dma((2, CHUNKS)),
            dma((2,)),
            dma((3 + SIZES[0] // HEAD_ROWS,)),
        ],
        compiler_params=pltpu.CompilerParams(
            collective_id=0, has_side_effects=True, vmem_limit_bytes=VMEM_ALL
        ),
        name="reduce_gradients",
    )(learn_rate, g_mat, g_vec, *params)


def adam_kernel(start, lr_ref, clip_ref, *refs):
    inputs, outputs, (wide, narrow, load_sem, store_sem) = refs[:4], refs[-8:-4], refs[-4:]
    count = narrow.shape[0] // ADAM_ROWS

    def rows(i, base=0):
        return pl.ds(pl.multiple_of(base + i * ADAM_ROWS, ADAM_ROWS), ADAM_ROWS)

    def load(k, i):
        return pltpu.make_async_copy(inputs[k].at[rows(i, start)], wide.at[k, rows(i)], load_sem.at[k, i])

    def store(k, i):
        if k == 3:
            return pltpu.make_async_copy(narrow.at[rows(i)], outputs[3].at[rows(i)], store_sem.at[3, i])
        return pltpu.make_async_copy(wide.at[k + 1, rows(i)], outputs[k].at[rows(i, start)], store_sem.at[k, i])

    for i in range(count):
        for k in range(4):
            load(k, i).start()

    def step(i, _):
        for k in range(4):
            load(k, i).wait()
        at = rows(i)
        grad = wide[0, at, :] * clip_ref[0:1, :]
        new_p, new_m, new_v = adam_update(grad, wide[1, at, :], wide[2, at, :], wide[3, at, :], lr_ref[0], WEIGHT_DECAY)
        wide[1, at, :] = new_p
        wide[2, at, :] = new_m
        wide[3, at, :] = new_v
        narrow[at, :] = new_p.astype(jnp.bfloat16)

        @pl.when(i > 0)
        def _():
            for k in (3, 0, 1, 2):
                store(k, i - 1).start()

        return 0

    lax.fori_loop(0, count, step, 0)
    for k in (3, 0, 1, 2):
        store(k, count - 1).start()
    for i in range(count):
        for k in range(4):
            store(k, i).wait()


def adam_chunk(start, size, learn_rate, clip, grad, params, state):
    hbm = pl.BlockSpec(memory_space=pltpu.HBM)
    whole = jax.ShapeDtypeStruct(grad.shape, jnp.float32)
    return pl.pallas_call(
        functools.partial(adam_kernel, start),
        out_shape=(whole, whole, whole, jax.ShapeDtypeStruct((size, LANES), jnp.bfloat16)),
        in_specs=[pl.BlockSpec(memory_space=pltpu.SMEM), pl.BlockSpec(memory_space=pltpu.VMEM)] + [hbm] * (4 + len(state)),
        out_specs=(hbm, hbm, hbm, hbm),
        input_output_aliases={6 + k: k for k in range(len(state))},
        scratch_shapes=[
            pltpu.VMEM((4, size, LANES), jnp.float32),
            pltpu.VMEM((size, LANES), jnp.bfloat16),
            pltpu.SemaphoreType.DMA((4, size // ADAM_ROWS)),
            pltpu.SemaphoreType.DMA((4, size // ADAM_ROWS)),
        ],
        cost_estimate=pl.CostEstimate(flops=size * LANES * 60, bytes_accessed=size * LANES * 30, transcendentals=0),
        compiler_params=pltpu.CompilerParams(vmem_limit_bytes=VMEM_ALL),
    )(learn_rate, clip, grad, *params, *state)


def place_kernel(axis_name, offsets, piece_rows, *refs):
    count = len(offsets)
    sources, out_ref, buffers, sems = refs[-2 * count - 3 : -count - 3], refs[-count - 3], refs[-count - 2 : -2], refs[-2:]
    _, core, x, y, dev = places(axis_name)
    owners = {"me": dev(y, x, core), "sib": dev(y, x, 1 - core),
              "x": dev(y, 1 - x, core), "x_sib": dev(y, 1 - x, 1 - core),
              "y": dev(1 - y, x, core), "y_sib": dev(1 - y, x, 1 - core),
              "d": dev(1 - y, 1 - x, core), "d_sib": dev(1 - y, 1 - x, 1 - core)}
    loads, stores = [], []
    for k, (who, start) in enumerate(offsets):
        size = sources[k].shape[0]
        at = pl.multiple_of(owners[who] * piece_rows + start, 16)
        loads.append(pltpu.make_async_copy(sources[k], buffers[k], sems[0].at[k]))
        stores.append(pltpu.make_async_copy(buffers[k], out_ref.at[pl.ds(at, size)], sems[1].at[k]))
    for load in loads:
        load.start()
    for load, store in zip(loads, stores):
        load.wait()
        store.start()
    for store in stores:
        store.wait()


def place(axis_name, piece_rows, full, items):
    hbm = pl.BlockSpec(memory_space=pltpu.HBM)
    sources = [source for _, _, source in items]
    moved = sum(source.shape[0] for source in sources)
    started = () if full is None else (full,)
    return pl.pallas_call(
        functools.partial(place_kernel, axis_name, tuple((who, start) for who, start, _ in items), piece_rows),
        out_shape=jax.ShapeDtypeStruct((DEVICES * piece_rows, LANES), jnp.bfloat16),
        in_specs=[hbm] * (len(started) + len(sources)),
        out_specs=hbm,
        input_output_aliases={0: 0} if started else {},
        scratch_shapes=[pltpu.VMEM(source.shape, jnp.bfloat16) for source in sources]
        + [pltpu.SemaphoreType.DMA((len(sources),))] * 2,
        cost_estimate=pl.CostEstimate(flops=moved * LANES * 15, bytes_accessed=moved * LANES * 4, transcendentals=0),
        compiler_params=pltpu.CompilerParams(vmem_limit_bytes=VMEM_ALL),
    )(*started, *sources)


def solution(mesh):
    axis_name = mesh.axis_names[0]
    to_sib = [(d, 4 * (d // 4) + 2 * (d // 2 % 2) + (1 - d % 2)) for d in range(DEVICES)]
    to_x = [(d, 4 * (d // 4) + 2 * (1 - d // 2 % 2) + d % 2) for d in range(DEVICES)]
    to_y = [(d, 4 * (1 - d // 4) + 2 * (d // 2 % 2) + d % 2) for d in range(DEVICES)]

    def move(array, pairs):
        return lax.ppermute(array, axis_name, pairs)

    def local_step(g_mat, g_vec, p_mat, m_mat, v_mat, p_vec, m_vec, v_vec, learn_rate):
        vec_size = g_vec.shape[1]
        params = [array.reshape(-1, LANES) for array in (p_mat, m_mat, v_mat)]
        piece_rows = params[0].shape[0]
        rate = learn_rate.reshape(1)
        grad_mat, grad_vec, clip, head, _ = reduce_gradients(axis_name, rate, g_mat, g_vec, params)

        starts = [sum(SIZES[:j]) for j in range(len(SIZES))]
        state, own = (), [head] * len(SIZES)
        for j in [*range(1, len(SIZES)), 0]:
            *state, narrow = adam_chunk(starts[j], SIZES[j], rate, clip, grad_mat, params, state)
            if j:
                own[j] = narrow

        sib, from_x, from_y = [], [], []
        for chunk in own:
            from_x.append(move(chunk, to_x))
            from_y.append(move(chunk, to_y))
            sib.append(move(chunk, to_sib))
        near, far = [], []
        for j, start in enumerate(starts):
            diag = move(from_y[j], to_x) if j % 2 == 0 else move(from_x[j], to_y)
            near.append([("me", start, own[j]), ("sib", start, sib[j]),
                         ("x", start, from_x[j]), ("x_sib", start, move(from_x[j], to_sib)),
                         ("y", start, from_y[j]), ("y_sib", start, move(from_y[j], to_sib))])
            far.append([("d", start, diag), ("d_sib", start, move(diag, to_sib))])
        full = None
        for group in NEAR_GROUPS:
            full = place(axis_name, piece_rows, full, sum((near[j] for j in group), []))
        for group in FAR_GROUPS:
            full = place(axis_name, piece_rows, full, sum((far[j] for j in group), []))

        grad_vec = grad_vec.reshape(-1)[:vec_size]
        new_p_vec, new_m_vec, new_v_vec = adam_update(grad_vec * clip[0, 0], p_vec, m_vec, v_vec, learn_rate, 0.0)
        new_p, new_m, new_v = (array.reshape(-1) for array in state)
        return new_p, new_m, new_v, new_p_vec, new_m_vec, new_v_vec, full.reshape(-1)

    return jax.shard_map(
        local_step,
        mesh=mesh,
        in_specs=(P(axis_name, None), P(axis_name, None), P(axis_name), P(axis_name), P(axis_name), P(), P(), P(), P()),
        out_specs=(P(axis_name), P(axis_name), P(axis_name), P(), P(), P(), P()),
        check_vma=False,
    )
```

```python
import functools

import jax
import jax.numpy as jnp
from jax import lax
from jax.experimental import pallas as pl
from jax.experimental.pallas import tpu as pltpu
from jax.sharding import PartitionSpec as P


STEP = 10
ADAM_BETA1 = 0.9
ADAM_BETA2 = 0.98
ADAM_EPS = 1e-8
WEIGHT_DECAY = 0.01
MAX_NORM = 1.0
NORM_EPS = 1e-6
BIAS_ONE = 1.0 - ADAM_BETA1 ** STEP
BIAS_TWO = 1.0 - ADAM_BETA2 ** STEP

MESH = pl.DeviceIdType.MESH
LANES = 128
DEVICES = 8
CHUNKS = 12
BLOCK = 160
ADAM_ROWS = 480
HEAD_ROWS = 480
SIZES = (1440, 2400, 4800, 4800, 2400, 1440, 960, 960)
NEAR_GROUPS = ((0, 1), (2,), (3,), (4, 5, 6, 7))
FAR_GROUPS = ((2, 3), (1, 4), (0, 5), (6, 7))
VMEM_ALL = 67043328
VMEM_DIRECT = 20971520


def adam_update(grad_vals, param_vals, moment_one, moment_two, learn_rate, decay_rate):
    new_one = ADAM_BETA1 * moment_one + (1.0 - ADAM_BETA1) * grad_vals
    new_two = ADAM_BETA2 * moment_two + (1.0 - ADAM_BETA2) * grad_vals * grad_vals
    direction = (new_one * (1.0 / BIAS_ONE)) / (jnp.sqrt(new_two * (1.0 / BIAS_TWO)) + ADAM_EPS)
    return param_vals - learn_rate * (direction + decay_rate * param_vals), new_one, new_two


def places(axis_name):
    me = lax.axis_index(axis_name)
    core, x, y = me % 2, (me // 2) % 2, me // 4

    def dev(yy, xx, cc):
        return 4 * yy + 2 * xx + cc

    return me, core, x, y, dev


def reduce_kernel(axis_name, half_rows, lr_ref, g_ref, gv_raw_ref, p_ref, m_ref, v_ref,
                  gsum_ref, vsum_ref, clip_ref, head_ref, stage_ref,
                  first, own_first, direct, own_direct, fsum, psum, raw, packed, vraw, vsend, vrecv, vpart, vall, nsend, nrecv,
                  clip, head_state, head,
                  vraw_sem, raw_sem, pack_sem, first_recv, direct_recv, psum_recv, send_sem, fsum_send,
                  vec_send, vec_recv, part_send, part_recv, nrm_send, nrm_recv, out_sem,
                  late_sem, head_sem):
    me, core, x, y, dev = places(axis_name)
    barrier = pltpu.get_barrier_semaphore()
    for o in range(1, DEVICES):
        pl.semaphore_signal(barrier, inc=1, device_id=((me + o) % DEVICES,), device_id_type=MESH)
    sib = dev(y, x, 1 - core)
    xs = [dev(y, 1 - x, 0), dev(y, 1 - x, 1)]
    ys = [dev(1 - y, x, 0), dev(1 - y, x, 1)]
    ds = [dev(1 - y, 1 - x, 0), dev(1 - y, 1 - x, 1)]
    x_mine, x_sib = dev(y, 1 - x, core), dev(y, 1 - x, 1 - core)
    y_mine, y_sib = dev(1 - y, x, core), dev(1 - y, x, 1 - core)
    rows = half_rows // CHUNKS
    vals = rows * LANES

    first_plan = [
        (2 * ds[0], ys[0], first, (0, core), first_recv),
        (2 * ds[0] + 1, xs[0], first, (1, core), first_recv),
        (2 * ds[1], ys[1], first, (0, core), first_recv),
        (2 * ds[1] + 1, xs[1], first, (1, core), first_recv),
        (2 * x_sib, sib, first, (0, 2), first_recv),
        (2 * y_sib + 1, sib, first, (1, 2), first_recv),
        (2 * x_mine, None, own_first, (0,), None),
        (2 * y_mine + 1, None, own_first, (1,), None),
    ]
    direct_plan = [
        (2 * ys[0], ys[0], direct, (0, core), direct_recv),
        (2 * xs[0] + 1, xs[0], direct, (1, core), direct_recv),
        (2 * ys[1], ys[1], direct, (0, core), direct_recv),
        (2 * xs[1] + 1, xs[1], direct, (1, core), direct_recv),
        (2 * sib, sib, direct, (0, 2), direct_recv),
        (2 * sib + 1, sib, direct, (1, 2), direct_recv),
        (2 * me, None, own_direct, (0,), None),
        (2 * me + 1, None, own_direct, (1,), None),
    ]

    def load_raw(plan, h, c):
        start = pl.multiple_of((plan[h][0] * CHUNKS + c) * vals, vals)
        return pltpu.make_async_copy(g_ref.at[:, pl.ds(start, vals)], raw.at[h], raw_sem.at[h])

    def stage_at(phase, h, c):
        return stage_ref.at[6 * phase + h, pl.ds(pl.multiple_of(c * rows, rows), rows), :]

    def to_stage(phase, h, c):
        return pltpu.make_async_copy(packed.at[h], stage_at(phase, h, c), pack_sem.at[h])

    def send(phase, plan, h, c):
        _, target, buf, slot, sems = plan[h]
        return pltpu.make_async_remote_copy(
            src_ref=stage_at(phase, h, c),
            dst_ref=buf.at[(*slot, pl.ds(pl.multiple_of(c * rows, rows), rows))],
            send_sem=send_sem.at[6 * phase + h],
            recv_sem=sems.at[slot],
            device_id=(target,),
            device_id_type=MESH,
        )

    def pack(plan, h, c):
        _, target, buf, slot, _ = plan[h]

        def body(i, _):
            piece = raw[h, :, pl.ds(pl.multiple_of(i * BLOCK * LANES, BLOCK * LANES), BLOCK * LANES)]
            piece = piece.astype(jnp.float32).reshape(BLOCK, LANES).astype(jnp.bfloat16)
            if target is None:
                buf[(*slot, pl.ds(pl.multiple_of(c * rows + i * BLOCK, BLOCK), BLOCK), slice(None))] = piece
            else:
                packed[h, pl.ds(pl.multiple_of(i * BLOCK, BLOCK), BLOCK), :] = piece
            return 0

        lax.fori_loop(0, rows // BLOCK, body, 0)

    vec_size, vec_rows = gv_raw_ref.shape[1], vsend.shape[1]
    vec_load = pltpu.make_async_copy(gv_raw_ref, vraw.at[:, pl.ds(0, vec_size)], vraw_sem)
    vec_load.start()
    for h in range(8):
        load_raw(first_plan, h, 0).start()
    vraw[:, vec_size:] = jnp.zeros((1, vraw.shape[1] - vec_size), jnp.bfloat16)
    vec_load.wait()
    vsend[...] = vraw[...].astype(jnp.float32).reshape(DEVICES, vec_rows, LANES).astype(jnp.bfloat16)
    vrecv[me] = vsend[me]

    def pack_all(phase, plan, next_plan, c):
        for h in range(8):
            load_raw(plan, h, c).wait()
            pack(plan, h, c)

            @pl.when(c + 1 < CHUNKS)
            def _():
                load_raw(plan, h, c + 1).start()

            if next_plan is not None:
                @pl.when(c + 1 >= CHUNKS)
                def _():
                    load_raw(next_plan, h, 0).start()

            if 1 <= h <= 6:
                to_stage(phase, h - 1, c).start()

    def send_all(phase, plan, c):
        for h in range(6):
            to_stage(phase, h, c).wait()
            send(phase, plan, h, c).start()

    def step(phase, plan, next_plan):
        def body(c, _):
            pack_all(phase, plan, next_plan, c)
            send_all(phase, plan, c)
            return 0

        return body

    pack_all(0, first_plan, direct_plan, 0)

    pl.semaphore_wait(barrier, DEVICES - 1)

    def vec_copy(o):
        target = (me + o) % DEVICES
        return pltpu.make_async_remote_copy(
            src_ref=vsend.at[target], dst_ref=vrecv.at[me], send_sem=vec_send.at[o], recv_sem=vec_recv.at[me],
            device_id=(target,), device_id_type=MESH)

    def part_copy(o):
        return pltpu.make_async_remote_copy(
            src_ref=vpart, dst_ref=vall.at[me], send_sem=part_send.at[o], recv_sem=part_recv.at[me],
            device_id=((me + o) % DEVICES,), device_id_type=MESH)

    def landed(buf, sems, o):
        src = (me + o) % DEVICES
        pltpu.make_async_copy(buf.at[src], buf.at[src], sems.at[src]).wait()

    for o in range(1, DEVICES):
        vec_copy(o).start()

    send_all(0, first_plan, 0)
    lax.fori_loop(1, CHUNKS, step(0, first_plan, direct_plan), 0)
    for o in range(1, DEVICES):
        landed(vrecv, vec_recv, o)
    vec_total = vrecv[0].astype(jnp.float32)
    for d in range(1, DEVICES):
        vec_total = vec_total + vrecv[d].astype(jnp.float32)
    vpart[...] = vec_total / DEVICES
    vall[me] = vec_total / DEVICES
    lax.fori_loop(0, CHUNKS, step(1, direct_plan, None), 0)
    for o in range(1, DEVICES):
        part_copy(o).start()

    def got_all(ref, sem):
        pltpu.make_async_copy(ref, ref, sem).wait()

    def fsum_copy(side, c):
        at = (side, pl.ds(pl.multiple_of(c * rows, rows), rows))
        return pltpu.make_async_remote_copy(
            src_ref=fsum.at[at], dst_ref=psum.at[at], send_sem=fsum_send.at[side], recv_sem=psum_recv.at[side, c],
            device_id=((x_mine, y_mine)[side],), device_id_type=MESH)

    for side in range(2):
        for slot in range(3):
            got_all(first.at[side, slot], first_recv.at[side, slot])

    def relay_step(c, _):
        for side in range(2):
            def body(i, _, side=side):
                at = pl.ds(pl.multiple_of(c * rows + i * BLOCK, BLOCK), BLOCK)
                total = first[side, 0, at, :].astype(jnp.float32) + first[side, 1, at, :].astype(jnp.float32)
                total = total + (first[side, 2, at, :].astype(jnp.float32) + own_first[side, at, :].astype(jnp.float32))
                fsum[side, at, :] = total
                return 0

            lax.fori_loop(0, rows // BLOCK, body, 0)
            if side == 1:
                fsum_copy(0, c).start()
            else:
                @pl.when(c > 0)
                def _():
                    fsum_copy(1, c - 1).start()
        return 0

    lax.fori_loop(0, CHUNKS, relay_step, 0)

    fsum_copy(1, CHUNKS - 1).start()
    for o in range(1, DEVICES):
        landed(vall, part_recv, o)
    vec_norm = jnp.sum((vall[...] * vall[...]).reshape(-1, 8, LANES), axis=0)
    vec_out = pltpu.make_async_copy(vall, vsum_ref, late_sem.at[0])
    vec_out.start()
    head_rows = head.shape[0]
    head_loads = [pltpu.make_async_copy(ref.at[pl.ds(0, head_rows)], head_state.at[k], head_sem.at[k])
                  for k, ref in enumerate((p_ref, m_ref, v_ref))]
    for load in head_loads:
        load.start()

    def out_copy(side, c):
        at = pl.ds(pl.multiple_of(c * rows, rows), rows)
        to = pl.ds(pl.multiple_of(side * half_rows + c * rows, rows), rows)
        return pltpu.make_async_copy(psum.at[side, at], gsum_ref.at[to], out_sem.at[side])

    def final_step(c, acc):
        for side in range(2):
            got_all(psum.at[side, pl.ds(pl.multiple_of(c * rows, rows), rows)], psum_recv.at[side, c])

            def body(i, acc, side=side):
                at = pl.ds(pl.multiple_of(c * rows + i * BLOCK, BLOCK), BLOCK)
                total = direct[side, 0, at, :].astype(jnp.float32) + direct[side, 1, at, :].astype(jnp.float32)
                total = total + (direct[side, 2, at, :].astype(jnp.float32) + own_direct[side, at, :].astype(jnp.float32))
                mean = (psum[side, at, :] + total) / DEVICES
                psum[side, at, :] = mean
                return acc + jnp.sum((mean * mean).reshape(BLOCK // 8, 8, LANES), axis=0)

            acc = lax.fori_loop(0, rows // BLOCK, body, acc)
            if side == 1:
                out_copy(0, c).start()
            else:
                @pl.when(c > 0)
                def _():
                    out_copy(1, c - 1).start()
        return acc

    for side in range(2):
        for slot in range(3):
            got_all(direct.at[side, slot], direct_recv.at[side, slot])
    acc = lax.fori_loop(0, CHUNKS, final_step, jnp.zeros((8, LANES), jnp.float32))
    nsend[...] = acc
    nrecv[me] = acc
    out_copy(1, CHUNKS - 1).start()

    for k in range(12):
        got_all(stage_ref.at[k], send_sem.at[k])

    def nrm_copy(o):
        return pltpu.make_async_remote_copy(
            src_ref=nsend, dst_ref=nrecv.at[me], send_sem=nrm_send.at[o], recv_sem=nrm_recv.at[me],
            device_id=((me + o) % DEVICES,), device_id_type=MESH)

    for o in range(1, DEVICES):
        nrm_copy(o).start()

    for side in range(2):
        got_all(fsum.at[side], fsum_send.at[side])
        got_all(psum.at[side], out_sem.at[side])
    for o in range(1, DEVICES):
        vec_copy(o).wait_send()
        part_copy(o).wait_send()
    for o in range(1, DEVICES):
        landed(nrecv, nrm_recv, o)
    tile = vec_norm
    for d in range(DEVICES):
        tile = tile + nrecv[d]
    norm_sq = jnp.full((8, LANES), jnp.sum(tile), jnp.float32)
    clip_tile = jnp.minimum(1.0, MAX_NORM / (jnp.sqrt(norm_sq) + NORM_EPS))
    clip[...] = clip_tile

    def head_copy(i):
        at = pl.ds(i * HEAD_ROWS, HEAD_ROWS)
        return pltpu.make_async_copy(head.at[at], head_ref.at[at], head_sem.at[3 + i])

    for load in head_loads:
        load.wait()
    clip_out = pltpu.make_async_copy(clip, clip_ref, late_sem.at[1])
    count = head_rows // HEAD_ROWS
    for i in range(count):
        at = pl.ds(i * HEAD_ROWS, HEAD_ROWS)
        new_p, _, _ = adam_update(psum[0, at, :] * clip_tile[0:1, :], head_state[0, at, :], head_state[1, at, :],
                                  head_state[2, at, :], lr_ref[0], WEIGHT_DECAY)
        head[at, :] = new_p.astype(jnp.bfloat16)
        if i == 0:
            clip_out.start()
        else:
            head_copy(i - 1).start()
    for o in range(1, DEVICES):
        nrm_copy(o).wait_send()
    vec_out.wait()
    head_copy(count - 1).start()
    clip_out.wait()
    for i in range(count):
        head_copy(i).wait()


def reduce_gradients(axis_name, learn_rate, g_mat, g_vec, params):
    half_rows = g_mat.shape[1] // (2 * DEVICES * LANES)
    rows = half_rows // CHUNKS
    vec_rows = -(-g_vec.shape[1] // (8 * LANES * DEVICES)) * 8
    bf16, f32 = jnp.bfloat16, jnp.float32
    dma = pltpu.SemaphoreType.DMA
    hbm = pl.BlockSpec(memory_space=pltpu.HBM)
    return pl.pallas_call(
        functools.partial(reduce_kernel, axis_name, half_rows),
        out_shape=(
            jax.ShapeDtypeStruct((2 * half_rows, LANES), f32),
            jax.ShapeDtypeStruct((DEVICES, vec_rows, LANES), f32),
            jax.ShapeDtypeStruct((8, LANES), f32),
            jax.ShapeDtypeStruct((SIZES[0], LANES), bf16),
            jax.ShapeDtypeStruct((12, half_rows, LANES), bf16),
        ),
        in_specs=[pl.BlockSpec(memory_space=pltpu.SMEM)] + [hbm] * 5,
        out_specs=(hbm,) * 5,
        scratch_shapes=[
            pltpu.VMEM((2, 3, half_rows, LANES), bf16),
            pltpu.VMEM((2, half_rows, LANES), bf16),
            pltpu.VMEM((2, 3, half_rows, LANES), bf16),
            pltpu.VMEM((2, half_rows, LANES), bf16),
            pltpu.VMEM((2, half_rows, LANES), f32),
            pltpu.VMEM((2, half_rows, LANES), f32),
            pltpu.VMEM((8, 1, rows * LANES), bf16),
            pltpu.VMEM((6, rows, LANES), bf16),
            pltpu.VMEM((1, DEVICES * vec_rows * LANES), bf16),
            pltpu.VMEM((DEVICES, vec_rows, LANES), bf16),
            pltpu.VMEM((DEVICES, vec_rows, LANES), bf16),
            pltpu.VMEM((vec_rows, LANES), f32),
            pltpu.VMEM((DEVICES, vec_rows, LANES), f32),
            pltpu.VMEM((8, LANES), f32),
            pltpu.VMEM((DEVICES, 8, LANES), f32),
            pltpu.VMEM((8, LANES), f32),
            pltpu.VMEM((3, SIZES[0], LANES), f32),
            pltpu.VMEM((SIZES[0], LANES), bf16),
            dma,
            dma((8,)),
            dma((6,)),
            dma((2, 3)),
            dma((2, 3)),
            dma((2, CHUNKS)),
            dma((12,)),
            dma((2,)),
            dma((DEVICES,)),
            dma((DEVICES,)),
            dma((DEVICES,)),
            dma((DEVICES,)),
            dma((DEVICES,)),
            dma((DEVICES,)),
            dma((2,)),
            dma((2,)),
            dma((3 + SIZES[0] // HEAD_ROWS,)),
        ],
        compiler_params=pltpu.CompilerParams(
            collective_id=0, has_side_effects=True, vmem_limit_bytes=VMEM_ALL
        ),
        name="reduce_gradients",
    )(learn_rate, g_mat, g_vec, *params)


def adam_kernel(start, lr_ref, clip_ref, *refs):
    inputs, outputs, (wide, narrow, load_sem, store_sem) = refs[:4], refs[-8:-4], refs[-4:]
    count = narrow.shape[0] // ADAM_ROWS

    def rows(i, base=0):
        return pl.ds(pl.multiple_of(base + i * ADAM_ROWS, ADAM_ROWS), ADAM_ROWS)

    def load(k, i):
        return pltpu.make_async_copy(inputs[k].at[rows(i, start)], wide.at[k, rows(i)], load_sem.at[k, i])

    def store(k, i):
        if k == 3:
            return pltpu.make_async_copy(narrow.at[rows(i)], outputs[3].at[rows(i)], store_sem.at[3, i])
        return pltpu.make_async_copy(wide.at[k + 1, rows(i)], outputs[k].at[rows(i, start)], store_sem.at[k, i])

    for i in range(count):
        for k in range(4):
            load(k, i).start()

    def step(i, _):
        for k in range(4):
            load(k, i).wait()
        at = rows(i)
        grad = wide[0, at, :] * clip_ref[0:1, :]
        new_p, new_m, new_v = adam_update(grad, wide[1, at, :], wide[2, at, :], wide[3, at, :], lr_ref[0], WEIGHT_DECAY)
        wide[1, at, :] = new_p
        wide[2, at, :] = new_m
        wide[3, at, :] = new_v
        narrow[at, :] = new_p.astype(jnp.bfloat16)

        @pl.when(i > 0)
        def _():
            for k in (3, 0, 1, 2):
                store(k, i - 1).start()

        return 0

    lax.fori_loop(0, count, step, 0)
    for k in (3, 0, 1, 2):
        store(k, count - 1).start()
    for i in range(count):
        for k in range(4):
            store(k, i).wait()


def adam_chunk(start, size, learn_rate, clip, grad, params, state):
    hbm = pl.BlockSpec(memory_space=pltpu.HBM)
    whole = jax.ShapeDtypeStruct(grad.shape, jnp.float32)
    return pl.pallas_call(
        functools.partial(adam_kernel, start),
        out_shape=(whole, whole, whole, jax.ShapeDtypeStruct((size, LANES), jnp.bfloat16)),
        in_specs=[pl.BlockSpec(memory_space=pltpu.SMEM), pl.BlockSpec(memory_space=pltpu.VMEM)] + [hbm] * (4 + len(state)),
        out_specs=(hbm, hbm, hbm, hbm),
        input_output_aliases={6 + k: k for k in range(len(state))},
        scratch_shapes=[
            pltpu.VMEM((4, size, LANES), jnp.float32),
            pltpu.VMEM((size, LANES), jnp.bfloat16),
            pltpu.SemaphoreType.DMA((4, size // ADAM_ROWS)),
            pltpu.SemaphoreType.DMA((4, size // ADAM_ROWS)),
        ],
        cost_estimate=pl.CostEstimate(flops=size * LANES * 60, bytes_accessed=size * LANES * 30, transcendentals=0),
        compiler_params=pltpu.CompilerParams(vmem_limit_bytes=VMEM_ALL),
    )(learn_rate, clip, grad, *params, *state)


def place_kernel(axis_name, offsets, piece_rows, direct, *refs):
    count = len(offsets)
    if direct:
        sources, out_ref, sem = refs[-count - 2 : -2], refs[-2], refs[-1]
    else:
        sources, out_ref, buffers, sems = refs[-2 * count - 3 : -count - 3], refs[-count - 3], refs[-count - 2 : -2], refs[-2:]
    _, core, x, y, dev = places(axis_name)
    owners = {"me": dev(y, x, core), "sib": dev(y, x, 1 - core),
              "x": dev(y, 1 - x, core), "x_sib": dev(y, 1 - x, 1 - core),
              "y": dev(1 - y, x, core), "y_sib": dev(1 - y, x, 1 - core),
              "d": dev(1 - y, 1 - x, core), "d_sib": dev(1 - y, 1 - x, 1 - core)}
    loads, stores = [], []
    for k, (who, start) in enumerate(offsets):
        size = sources[k].shape[0]
        at = pl.multiple_of(owners[who] * piece_rows + start, 16)
        if direct:
            stores.append(pltpu.make_async_copy(sources[k], out_ref.at[pl.ds(at, size)], sem.at[k]))
            continue
        loads.append(pltpu.make_async_copy(sources[k], buffers[k], sems[0].at[k]))
        stores.append(pltpu.make_async_copy(buffers[k], out_ref.at[pl.ds(at, size)], sems[1].at[k]))
    for load in loads:
        load.start()
    for k, store in enumerate(stores):
        if not direct:
            loads[k].wait()
        store.start()
    for store in stores:
        store.wait()


def place(axis_name, piece_rows, full, items, name, direct=False):
    hbm = pl.BlockSpec(memory_space=pltpu.HBM)
    sources = [source for _, _, source in items]
    moved = sum(source.shape[0] for source in sources)
    started = () if full is None else (full,)
    return pl.pallas_call(
        functools.partial(place_kernel, axis_name, tuple((who, start) for who, start, _ in items), piece_rows, direct),
        out_shape=jax.ShapeDtypeStruct((DEVICES * piece_rows, LANES), jnp.bfloat16),
        in_specs=[hbm] * len(started) + [pl.BlockSpec(memory_space=pltpu.VMEM) if direct else hbm] * len(sources),
        out_specs=hbm,
        input_output_aliases={0: 0} if started else {},
        scratch_shapes=[pltpu.VMEM(source.shape, jnp.bfloat16) for source in sources if not direct]
        + [pltpu.SemaphoreType.DMA((len(sources),))] * (1 if direct else 2),
        cost_estimate=pl.CostEstimate(flops=moved * LANES * 15, bytes_accessed=moved * LANES * 4, transcendentals=0),
        compiler_params=pltpu.CompilerParams(vmem_limit_bytes=VMEM_DIRECT if direct or name == "near_3" else VMEM_ALL),
    )(*started, *sources)


def solution(mesh):
    axis_name = mesh.axis_names[0]
    to_sib = [(d, 4 * (d // 4) + 2 * (d // 2 % 2) + (1 - d % 2)) for d in range(DEVICES)]
    to_x = [(d, 4 * (d // 4) + 2 * (1 - d // 2 % 2) + d % 2) for d in range(DEVICES)]
    to_y = [(d, 4 * (1 - d // 4) + 2 * (d // 2 % 2) + d % 2) for d in range(DEVICES)]

    def move(array, pairs):
        return lax.ppermute(array, axis_name, pairs)

    def local_step(g_mat, g_vec, p_mat, m_mat, v_mat, p_vec, m_vec, v_vec, learn_rate):
        vec_size = g_vec.shape[1]
        params = [array.reshape(-1, LANES) for array in (p_mat, m_mat, v_mat)]
        piece_rows = params[0].shape[0]
        rate = learn_rate.reshape(1)
        grad_mat, grad_vec, clip, head, _ = reduce_gradients(axis_name, rate, g_mat, g_vec, params)

        starts = [sum(SIZES[:j]) for j in range(len(SIZES))]
        state, own = (), [head] * len(SIZES)
        for j in [*range(1, len(SIZES)), 0]:
            *state, narrow = adam_chunk(starts[j], SIZES[j], rate, clip, grad_mat, params, state)
            if j:
                own[j] = narrow

        sib, from_x, from_y = [], [], []
        for chunk in own:
            from_x.append(move(chunk, to_x))
            from_y.append(move(chunk, to_y))
            sib.append(move(chunk, to_sib))
        near, far = [], []
        for j, start in enumerate(starts):
            diag = move(from_y[j], to_x) if j % 2 == 0 else move(from_x[j], to_y)
            near.append([("me", start, own[j]), ("sib", start, sib[j]),
                         ("x", start, from_x[j]), ("x_sib", start, move(from_x[j], to_sib)),
                         ("y", start, from_y[j]), ("y_sib", start, move(from_y[j], to_sib))])
            far.append([("d", start, diag), ("d_sib", start, move(diag, to_sib))])
        full = None
        for k, group in enumerate(NEAR_GROUPS):
            full = place(axis_name, piece_rows, full, sum((near[j] for j in group), []), f"near_{k}")
        for k, group in enumerate(FAR_GROUPS):
            full = place(axis_name, piece_rows, full, sum((far[j] for j in group), []), f"far_{k}",
                         direct=True)

        grad_vec = grad_vec.reshape(-1)[:vec_size]
        new_p_vec, new_m_vec, new_v_vec = adam_update(grad_vec * clip[0, 0], p_vec, m_vec, v_vec, learn_rate, 0.0)
        new_p, new_m, new_v = (array.reshape(-1) for array in state)
        return new_p, new_m, new_v, new_p_vec, new_m_vec, new_v_vec, full.reshape(-1)

    return jax.shard_map(
        local_step,
        mesh=mesh,
        in_specs=(P(axis_name, None), P(axis_name, None), P(axis_name), P(axis_name), P(axis_name), P(), P(), P(), P()),
        out_specs=(P(axis_name), P(axis_name), P(axis_name), P(), P(), P(), P()),
        check_vma=False,
    )
```

```python
import functools

import jax
import jax.numpy as jnp
from jax import lax
from jax.experimental import pallas as pl
from jax.experimental.pallas import tpu as pltpu
from jax.sharding import PartitionSpec as P


STEP = 10
ADAM_BETA1 = 0.9
ADAM_BETA2 = 0.98
ADAM_EPS = 1e-8
WEIGHT_DECAY = 0.01
MAX_NORM = 1.0
NORM_EPS = 1e-6
BIAS_ONE = 1.0 - ADAM_BETA1 ** STEP
BIAS_TWO = 1.0 - ADAM_BETA2 ** STEP

MESH = pl.DeviceIdType.MESH
LANES = 128
DEVICES = 8
CHUNKS = 15
BLOCK = 160
ADAM_ROWS = 480
HEAD_ROWS = 480
SIZES = (1440, 2400, 4800, 4800, 2400, 1440, 960, 960)
NEAR_GROUPS = ((0, 1), (2,), (3,), (4, 5, 6, 7))
FAR_GROUPS = ((2, 3), (1, 4), (0, 5), (6, 7))
VMEM_ALL = 67043328
VMEM_DIRECT = 20971520


def adam_update(grad_vals, param_vals, moment_one, moment_two, learn_rate, decay_rate):
    new_one = ADAM_BETA1 * moment_one + (1.0 - ADAM_BETA1) * grad_vals
    new_two = ADAM_BETA2 * moment_two + (1.0 - ADAM_BETA2) * grad_vals * grad_vals
    direction = (new_one * (1.0 / BIAS_ONE)) / (jnp.sqrt(new_two * (1.0 / BIAS_TWO)) + ADAM_EPS)
    return param_vals - learn_rate * (direction + decay_rate * param_vals), new_one, new_two


def places(axis_name):
    me = lax.axis_index(axis_name)
    core, x, y = me % 2, (me // 2) % 2, me // 4

    def dev(yy, xx, cc):
        return 4 * yy + 2 * xx + cc

    return me, core, x, y, dev


def reduce_kernel(axis_name, half_rows, lr_ref, g_ref, gv_raw_ref, p_ref, m_ref, v_ref,
                  gsum_ref, vsum_ref, clip_ref, head_ref, stage_ref,
                  first, own_first, direct, own_direct, fsum, psum, raw, packed, vraw, vsend, vrecv, vpart, vall, nsend, nrecv,
                  clip, head_state, head,
                  vraw_sem, raw_sem, pack_sem, first_recv, direct_recv, psum_recv, send_sem, fsum_send,
                  vec_send, vec_recv, part_send, part_recv, nrm_send, nrm_recv, out_sem,
                  late_sem, head_sem):
    me, core, x, y, dev = places(axis_name)
    barrier = pltpu.get_barrier_semaphore()
    for o in range(1, DEVICES):
        pl.semaphore_signal(barrier, inc=1, device_id=((me + o) % DEVICES,), device_id_type=MESH)
    sib = dev(y, x, 1 - core)
    xs = [dev(y, 1 - x, 0), dev(y, 1 - x, 1)]
    ys = [dev(1 - y, x, 0), dev(1 - y, x, 1)]
    ds = [dev(1 - y, 1 - x, 0), dev(1 - y, 1 - x, 1)]
    x_mine, x_sib = dev(y, 1 - x, core), dev(y, 1 - x, 1 - core)
    y_mine, y_sib = dev(1 - y, x, core), dev(1 - y, x, 1 - core)
    rows = half_rows // CHUNKS
    vals = rows * LANES

    first_plan = [
        (2 * ds[0], ys[0], first, (0, core), first_recv),
        (2 * ds[0] + 1, xs[0], first, (1, core), first_recv),
        (2 * ds[1], ys[1], first, (0, core), first_recv),
        (2 * ds[1] + 1, xs[1], first, (1, core), first_recv),
        (2 * x_sib, sib, first, (0, 2), first_recv),
        (2 * y_sib + 1, sib, first, (1, 2), first_recv),
        (2 * x_mine, None, own_first, (0,), None),
        (2 * y_mine + 1, None, own_first, (1,), None),
    ]
    direct_plan = [
        (2 * ys[0], ys[0], direct, (0, core), direct_recv),
        (2 * xs[0] + 1, xs[0], direct, (1, core), direct_recv),
        (2 * ys[1], ys[1], direct, (0, core), direct_recv),
        (2 * xs[1] + 1, xs[1], direct, (1, core), direct_recv),
        (2 * sib, sib, direct, (0, 2), direct_recv),
        (2 * sib + 1, sib, direct, (1, 2), direct_recv),
        (2 * me, None, own_direct, (0,), None),
        (2 * me + 1, None, own_direct, (1,), None),
    ]

    def load_raw(plan, h, c):
        start = pl.multiple_of((plan[h][0] * CHUNKS + c) * vals, vals)
        return pltpu.make_async_copy(g_ref.at[:, pl.ds(start, vals)], raw.at[h], raw_sem.at[h])

    def stage_at(phase, h, c):
        return stage_ref.at[6 * phase + h, pl.ds(pl.multiple_of(c * rows, rows), rows), :]

    def to_stage(phase, h, c):
        return pltpu.make_async_copy(packed.at[h], stage_at(phase, h, c), pack_sem.at[h])

    def send(phase, plan, h, c):
        _, target, buf, slot, sems = plan[h]
        return pltpu.make_async_remote_copy(
            src_ref=stage_at(phase, h, c),
            dst_ref=buf.at[(*slot, pl.ds(pl.multiple_of(c * rows, rows), rows))],
            send_sem=send_sem.at[6 * phase + h],
            recv_sem=sems.at[slot],
            device_id=(target,),
            device_id_type=MESH,
        )

    def pack(plan, h, c):
        _, target, buf, slot, _ = plan[h]

        def body(i, _):
            piece = raw[h, :, pl.ds(pl.multiple_of(i * BLOCK * LANES, BLOCK * LANES), BLOCK * LANES)]
            piece = piece.astype(jnp.float32).reshape(BLOCK, LANES).astype(jnp.bfloat16)
            if target is None:
                buf[(*slot, pl.ds(pl.multiple_of(c * rows + i * BLOCK, BLOCK), BLOCK), slice(None))] = piece
            else:
                packed[h, pl.ds(pl.multiple_of(i * BLOCK, BLOCK), BLOCK), :] = piece
            return 0

        lax.fori_loop(0, rows // BLOCK, body, 0)

    vec_size, vec_rows = gv_raw_ref.shape[1], vsend.shape[1]
    vec_load = pltpu.make_async_copy(gv_raw_ref, vraw.at[:, pl.ds(0, vec_size)], vraw_sem)
    vec_load.start()
    for h in range(8):
        load_raw(first_plan, h, 0).start()
    vraw[:, vec_size:] = jnp.zeros((1, vraw.shape[1] - vec_size), jnp.bfloat16)
    vec_load.wait()
    vsend[...] = vraw[...].astype(jnp.float32).reshape(DEVICES, vec_rows, LANES).astype(jnp.bfloat16)
    vrecv[me] = vsend[me]

    def pack_units(phase, plan, next_plan, c, units):
        for h in units:
            load_raw(plan, h, c).wait()
            pack(plan, h, c)

            @pl.when(c + 1 < CHUNKS)
            def _():
                load_raw(plan, h, c + 1).start()

            if next_plan is not None:
                @pl.when(c + 1 >= CHUNKS)
                def _():
                    load_raw(next_plan, h, 0).start()

            if h - 1 in units and h <= 6:
                to_stage(phase, h - 1, c).start()

    def send_units(phase, plan, c, units):
        for h in units:
            to_stage(phase, h, c).wait()
            send(phase, plan, h, c).start()

    def step(phase, plan, next_plan):
        def body(c, _):
            pack_units(phase, plan, next_plan, c, range(8))
            send_units(phase, plan, c, range(6))
            return 0

        return body

    pack_units(0, first_plan, direct_plan, 0, range(4))

    pl.semaphore_wait(barrier, DEVICES - 1)

    def vec_copy(o):
        target = (me + o) % DEVICES
        return pltpu.make_async_remote_copy(
            src_ref=vsend.at[target], dst_ref=vrecv.at[me], send_sem=vec_send.at[o], recv_sem=vec_recv.at[me],
            device_id=(target,), device_id_type=MESH)

    partners = [dev(1 - y, 1 - x, core), y_mine, x_mine, sib]

    def part_copy(k):
        return pltpu.make_async_remote_copy(
            src_ref=vpart, dst_ref=vall.at[me], send_sem=part_send.at[k], recv_sem=part_recv.at[me],
            device_id=(partners[k],), device_id_type=MESH)

    def part_pass(k):
        return pltpu.make_async_remote_copy(
            src_ref=vall.at[partners[k]], dst_ref=vall.at[partners[k]], send_sem=part_send.at[4 + k],
            recv_sem=part_recv.at[partners[k]], device_id=(sib,), device_id_type=MESH)

    def part_landed(src):
        pltpu.make_async_copy(vall.at[src], vall.at[src], part_recv.at[src]).wait()

    def landed(buf, sems, o):
        src = (me + o) % DEVICES
        pltpu.make_async_copy(buf.at[src], buf.at[src], sems.at[src]).wait()

    to_stage(0, 3, 0).start()
    send_units(0, first_plan, 0, range(4))
    for o in range(1, DEVICES):
        vec_copy(o).start()

    pack_units(0, first_plan, direct_plan, 0, range(4, 8))
    send_units(0, first_plan, 0, range(4, 6))
    lax.fori_loop(1, CHUNKS, step(0, first_plan, direct_plan), 0)
    for o in range(1, DEVICES):
        landed(vrecv, vec_recv, o)
    vec_total = vrecv[0].astype(jnp.float32)
    for d in range(1, DEVICES):
        vec_total = vec_total + vrecv[d].astype(jnp.float32)
    vpart[...] = vec_total / DEVICES
    vall[me] = vec_total / DEVICES
    lax.fori_loop(0, CHUNKS, step(1, direct_plan, None), 0)
    for k in range(4):
        part_copy(k).start()

    def got_all(ref, sem):
        pltpu.make_async_copy(ref, ref, sem).wait()

    def fsum_copy(side, c):
        at = (side, pl.ds(pl.multiple_of(c * rows, rows), rows))
        return pltpu.make_async_remote_copy(
            src_ref=fsum.at[at], dst_ref=psum.at[at], send_sem=fsum_send.at[side], recv_sem=psum_recv.at[side, c],
            device_id=((x_mine, y_mine)[side],), device_id_type=MESH)

    for side in range(2):
        for slot in range(3):
            got_all(first.at[side, slot], first_recv.at[side, slot])

    def relay_step(c, _):
        for side in range(2):
            def body(i, _, side=side):
                at = pl.ds(pl.multiple_of(c * rows + i * BLOCK, BLOCK), BLOCK)
                total = first[side, 0, at, :].astype(jnp.float32) + first[side, 1, at, :].astype(jnp.float32)
                total = total + (first[side, 2, at, :].astype(jnp.float32) + own_first[side, at, :].astype(jnp.float32))
                fsum[side, at, :] = total
                return 0

            lax.fori_loop(0, rows // BLOCK, body, 0)
            if side == 1:
                fsum_copy(0, c).start()
            else:
                @pl.when(c > 0)
                def _():
                    fsum_copy(1, c - 1).start()
        return 0

    lax.fori_loop(0, CHUNKS, relay_step, 0)

    fsum_copy(1, CHUNKS - 1).start()
    for k in range(3):
        part_landed(partners[k])
        part_pass(k).start()
    part_landed(sib)
    for side in range(2):
        for slot in range(3):
            got_all(direct.at[side, slot], direct_recv.at[side, slot])
    for other in (x_sib, y_sib, dev(1 - y, 1 - x, 1 - core)):
        part_landed(other)
    vec_norm = jnp.sum((vall[...] * vall[...]).reshape(-1, 8, LANES), axis=0)
    vec_out = pltpu.make_async_copy(vall, vsum_ref, late_sem.at[0])
    vec_out.start()
    head_rows = head.shape[0]
    head_loads = [pltpu.make_async_copy(ref.at[pl.ds(0, head_rows)], head_state.at[k], head_sem.at[k])
                  for k, ref in enumerate((p_ref, m_ref, v_ref))]
    for load in head_loads:
        load.start()

    def out_copy(side, c):
        at = pl.ds(pl.multiple_of(c * rows, rows), rows)
        to = pl.ds(pl.multiple_of(side * half_rows + c * rows, rows), rows)
        return pltpu.make_async_copy(psum.at[side, at], gsum_ref.at[to], out_sem.at[side])

    def final_step(c, acc):
        for side in range(2):
            got_all(psum.at[side, pl.ds(pl.multiple_of(c * rows, rows), rows)], psum_recv.at[side, c])

            def body(i, acc, side=side):
                at = pl.ds(pl.multiple_of(c * rows + i * BLOCK, BLOCK), BLOCK)
                total = direct[side, 0, at, :].astype(jnp.float32) + direct[side, 1, at, :].astype(jnp.float32)
                total = total + (direct[side, 2, at, :].astype(jnp.float32) + own_direct[side, at, :].astype(jnp.float32))
                mean = (psum[side, at, :] + total) / DEVICES
                psum[side, at, :] = mean
                return acc + jnp.sum((mean * mean).reshape(BLOCK // 8, 8, LANES), axis=0)

            acc = lax.fori_loop(0, rows // BLOCK, body, acc)
            if side == 1:
                out_copy(0, c).start()
            else:
                @pl.when(c > 0)
                def _():
                    out_copy(1, c - 1).start()
        return acc

    acc = lax.fori_loop(0, CHUNKS, final_step, jnp.zeros((8, LANES), jnp.float32))
    nsend[...] = acc
    nrecv[me] = acc
    out_copy(1, CHUNKS - 1).start()

    for k in range(12):
        got_all(stage_ref.at[k], send_sem.at[k])

    def nrm_copy(o):
        return pltpu.make_async_remote_copy(
            src_ref=nsend, dst_ref=nrecv.at[me], send_sem=nrm_send.at[o], recv_sem=nrm_recv.at[me],
            device_id=((me + o) % DEVICES,), device_id_type=MESH)

    for o in range(1, DEVICES):
        nrm_copy(o).start()

    for side in range(2):
        got_all(fsum.at[side], fsum_send.at[side])
        got_all(psum.at[side], out_sem.at[side])
    for o in range(1, DEVICES):
        vec_copy(o).wait_send()
    for k in range(4):
        part_copy(k).wait_send()
    for k in range(3):
        part_pass(k).wait_send()
    for o in range(1, DEVICES):
        landed(nrecv, nrm_recv, o)
    tile = vec_norm
    for d in range(DEVICES):
        tile = tile + nrecv[d]
    norm_sq = jnp.full((8, LANES), jnp.sum(tile), jnp.float32)
    clip_tile = jnp.minimum(1.0, MAX_NORM / (jnp.sqrt(norm_sq) + NORM_EPS))
    clip[...] = clip_tile

    def head_copy(i):
        at = pl.ds(i * HEAD_ROWS, HEAD_ROWS)
        return pltpu.make_async_copy(head.at[at], head_ref.at[at], head_sem.at[3 + i])

    for load in head_loads:
        load.wait()
    clip_out = pltpu.make_async_copy(clip, clip_ref, late_sem.at[1])
    count = head_rows // HEAD_ROWS
    for i in range(count):
        at = pl.ds(i * HEAD_ROWS, HEAD_ROWS)
        new_p, _, _ = adam_update(psum[0, at, :] * clip_tile[0:1, :], head_state[0, at, :], head_state[1, at, :],
                                  head_state[2, at, :], lr_ref[0], WEIGHT_DECAY)
        head[at, :] = new_p.astype(jnp.bfloat16)
        if i == 0:
            clip_out.start()
        else:
            head_copy(i - 1).start()
    for o in range(1, DEVICES):
        nrm_copy(o).wait_send()
    vec_out.wait()
    head_copy(count - 1).start()
    clip_out.wait()
    for i in range(count):
        head_copy(i).wait()


def reduce_gradients(axis_name, learn_rate, g_mat, g_vec, params):
    half_rows = g_mat.shape[1] // (2 * DEVICES * LANES)
    rows = half_rows // CHUNKS
    vec_rows = -(-g_vec.shape[1] // (8 * LANES * DEVICES)) * 8
    bf16, f32 = jnp.bfloat16, jnp.float32
    dma = pltpu.SemaphoreType.DMA
    hbm = pl.BlockSpec(memory_space=pltpu.HBM)
    return pl.pallas_call(
        functools.partial(reduce_kernel, axis_name, half_rows),
        out_shape=(
            jax.ShapeDtypeStruct((2 * half_rows, LANES), f32),
            jax.ShapeDtypeStruct((DEVICES, vec_rows, LANES), f32),
            jax.ShapeDtypeStruct((8, LANES), f32),
            jax.ShapeDtypeStruct((SIZES[0], LANES), bf16),
            jax.ShapeDtypeStruct((12, half_rows, LANES), bf16),
        ),
        in_specs=[pl.BlockSpec(memory_space=pltpu.SMEM)] + [hbm] * 5,
        out_specs=(hbm,) * 5,
        scratch_shapes=[
            pltpu.VMEM((2, 3, half_rows, LANES), bf16),
            pltpu.VMEM((2, half_rows, LANES), bf16),
            pltpu.VMEM((2, 3, half_rows, LANES), bf16),
            pltpu.VMEM((2, half_rows, LANES), bf16),
            pltpu.VMEM((2, half_rows, LANES), f32),
            pltpu.VMEM((2, half_rows, LANES), f32),
            pltpu.VMEM((8, 1, rows * LANES), bf16),
            pltpu.VMEM((6, rows, LANES), bf16),
            pltpu.VMEM((1, DEVICES * vec_rows * LANES), bf16),
            pltpu.VMEM((DEVICES, vec_rows, LANES), bf16),
            pltpu.VMEM((DEVICES, vec_rows, LANES), bf16),
            pltpu.VMEM((vec_rows, LANES), f32),
            pltpu.VMEM((DEVICES, vec_rows, LANES), f32),
            pltpu.VMEM((8, LANES), f32),
            pltpu.VMEM((DEVICES, 8, LANES), f32),
            pltpu.VMEM((8, LANES), f32),
            pltpu.VMEM((3, SIZES[0], LANES), f32),
            pltpu.VMEM((SIZES[0], LANES), bf16),
            dma,
            dma((8,)),
            dma((6,)),
            dma((2, 3)),
            dma((2, 3)),
            dma((2, CHUNKS)),
            dma((12,)),
            dma((2,)),
            dma((DEVICES,)),
            dma((DEVICES,)),
            dma((DEVICES,)),
            dma((DEVICES,)),
            dma((DEVICES,)),
            dma((DEVICES,)),
            dma((2,)),
            dma((2,)),
            dma((3 + SIZES[0] // HEAD_ROWS,)),
        ],
        compiler_params=pltpu.CompilerParams(
            collective_id=0, has_side_effects=True, vmem_limit_bytes=VMEM_ALL
        ),
        name="reduce_gradients",
    )(learn_rate, g_mat, g_vec, *params)


def adam_kernel(start, lr_ref, clip_ref, *refs):
    inputs, outputs, (wide, narrow, load_sem, store_sem) = refs[:4], refs[-8:-4], refs[-4:]
    count = narrow.shape[0] // ADAM_ROWS

    def rows(i, base=0):
        return pl.ds(pl.multiple_of(base + i * ADAM_ROWS, ADAM_ROWS), ADAM_ROWS)

    def load(k, i):
        return pltpu.make_async_copy(inputs[k].at[rows(i, start)], wide.at[k, rows(i)], load_sem.at[k, i])

    def store(k, i):
        if k == 3:
            return pltpu.make_async_copy(narrow.at[rows(i)], outputs[3].at[rows(i)], store_sem.at[3, i])
        return pltpu.make_async_copy(wide.at[k + 1, rows(i)], outputs[k].at[rows(i, start)], store_sem.at[k, i])

    for i in range(count):
        for k in range(4):
            load(k, i).start()

    def step(i, _):
        for k in range(4):
            load(k, i).wait()
        at = rows(i)
        grad = wide[0, at, :] * clip_ref[0:1, :]
        new_p, new_m, new_v = adam_update(grad, wide[1, at, :], wide[2, at, :], wide[3, at, :], lr_ref[0], WEIGHT_DECAY)
        wide[1, at, :] = new_p
        wide[2, at, :] = new_m
        wide[3, at, :] = new_v
        narrow[at, :] = new_p.astype(jnp.bfloat16)

        @pl.when(i > 0)
        def _():
            for k in (3, 0, 1, 2):
                store(k, i - 1).start()

        return 0

    lax.fori_loop(0, count, step, 0)
    for k in (3, 0, 1, 2):
        store(k, count - 1).start()
    for i in range(count):
        for k in range(4):
            store(k, i).wait()


def adam_chunk(start, size, learn_rate, clip, grad, params, state):
    hbm = pl.BlockSpec(memory_space=pltpu.HBM)
    whole = jax.ShapeDtypeStruct(grad.shape, jnp.float32)
    return pl.pallas_call(
        functools.partial(adam_kernel, start),
        out_shape=(whole, whole, whole, jax.ShapeDtypeStruct((size, LANES), jnp.bfloat16)),
        in_specs=[pl.BlockSpec(memory_space=pltpu.SMEM), pl.BlockSpec(memory_space=pltpu.VMEM)] + [hbm] * (4 + len(state)),
        out_specs=(hbm, hbm, hbm, hbm),
        input_output_aliases={6 + k: k for k in range(len(state))},
        scratch_shapes=[
            pltpu.VMEM((4, size, LANES), jnp.float32),
            pltpu.VMEM((size, LANES), jnp.bfloat16),
            pltpu.SemaphoreType.DMA((4, size // ADAM_ROWS)),
            pltpu.SemaphoreType.DMA((4, size // ADAM_ROWS)),
        ],
        cost_estimate=pl.CostEstimate(flops=size * LANES * 60, bytes_accessed=size * LANES * 30, transcendentals=0),
        compiler_params=pltpu.CompilerParams(vmem_limit_bytes=VMEM_ALL),
    )(learn_rate, clip, grad, *params, *state)


def place_kernel(axis_name, offsets, piece_rows, direct, *refs):
    count = len(offsets)
    if direct:
        sources, out_ref, sem = refs[-count - 2 : -2], refs[-2], refs[-1]
    else:
        sources, out_ref, buffers, sems = refs[-2 * count - 3 : -count - 3], refs[-count - 3], refs[-count - 2 : -2], refs[-2:]
    _, core, x, y, dev = places(axis_name)
    owners = {"me": dev(y, x, core), "sib": dev(y, x, 1 - core),
              "x": dev(y, 1 - x, core), "x_sib": dev(y, 1 - x, 1 - core),
              "y": dev(1 - y, x, core), "y_sib": dev(1 - y, x, 1 - core),
              "d": dev(1 - y, 1 - x, core), "d_sib": dev(1 - y, 1 - x, 1 - core)}
    loads, stores = [], []
    for k, (who, start) in enumerate(offsets):
        size = sources[k].shape[0]
        at = pl.multiple_of(owners[who] * piece_rows + start, 16)
        if direct:
            stores.append(pltpu.make_async_copy(sources[k], out_ref.at[pl.ds(at, size)], sem.at[k]))
            continue
        loads.append(pltpu.make_async_copy(sources[k], buffers[k], sems[0].at[k]))
        stores.append(pltpu.make_async_copy(buffers[k], out_ref.at[pl.ds(at, size)], sems[1].at[k]))
    for load in loads:
        load.start()
    for k, store in enumerate(stores):
        if not direct:
            loads[k].wait()
        store.start()
    for store in stores:
        store.wait()


def place(axis_name, piece_rows, full, items, name, direct=False):
    hbm = pl.BlockSpec(memory_space=pltpu.HBM)
    sources = [source for _, _, source in items]
    moved = sum(source.shape[0] for source in sources)
    started = () if full is None else (full,)
    return pl.pallas_call(
        functools.partial(place_kernel, axis_name, tuple((who, start) for who, start, _ in items), piece_rows, direct),
        out_shape=jax.ShapeDtypeStruct((DEVICES * piece_rows, LANES), jnp.bfloat16),
        in_specs=[hbm] * len(started) + [pl.BlockSpec(memory_space=pltpu.VMEM) if direct else hbm] * len(sources),
        out_specs=hbm,
        input_output_aliases={0: 0} if started else {},
        scratch_shapes=[pltpu.VMEM(source.shape, jnp.bfloat16) for source in sources if not direct]
        + [pltpu.SemaphoreType.DMA((len(sources),))] * (1 if direct else 2),
        cost_estimate=pl.CostEstimate(flops=moved * LANES * 15, bytes_accessed=moved * LANES * 4, transcendentals=0),
        compiler_params=pltpu.CompilerParams(vmem_limit_bytes=VMEM_DIRECT if direct or name == "near_3" else VMEM_ALL),
    )(*started, *sources)


def solution(mesh):
    axis_name = mesh.axis_names[0]
    to_sib = [(d, 4 * (d // 4) + 2 * (d // 2 % 2) + (1 - d % 2)) for d in range(DEVICES)]
    to_x = [(d, 4 * (d // 4) + 2 * (1 - d // 2 % 2) + d % 2) for d in range(DEVICES)]
    to_y = [(d, 4 * (1 - d // 4) + 2 * (d // 2 % 2) + d % 2) for d in range(DEVICES)]

    def move(array, pairs):
        return lax.ppermute(array, axis_name, pairs)

    def local_step(g_mat, g_vec, p_mat, m_mat, v_mat, p_vec, m_vec, v_vec, learn_rate):
        vec_size = g_vec.shape[1]
        params = [array.reshape(-1, LANES) for array in (p_mat, m_mat, v_mat)]
        piece_rows = params[0].shape[0]
        rate = learn_rate.reshape(1)
        grad_mat, grad_vec, clip, head, _ = reduce_gradients(axis_name, rate, g_mat, g_vec, params)

        starts = [sum(SIZES[:j]) for j in range(len(SIZES))]
        state, own = (), [head] * len(SIZES)
        for j in [*range(1, len(SIZES)), 0]:
            *state, narrow = adam_chunk(starts[j], SIZES[j], rate, clip, grad_mat, params, state)
            if j:
                own[j] = narrow

        sib, from_x, from_y = [], [], []
        for chunk in own:
            from_x.append(move(chunk, to_x))
            from_y.append(move(chunk, to_y))
            sib.append(move(chunk, to_sib))
        near, far = [], []
        for j, start in enumerate(starts):
            diag = move(from_y[j], to_x) if j % 2 == 0 else move(from_x[j], to_y)
            near.append([("me", start, own[j]), ("sib", start, sib[j]),
                         ("x", start, from_x[j]), ("x_sib", start, move(from_x[j], to_sib)),
                         ("y", start, from_y[j]), ("y_sib", start, move(from_y[j], to_sib))])
            far.append([("d", start, diag), ("d_sib", start, move(diag, to_sib))])
        full = None
        for k, group in enumerate(NEAR_GROUPS):
            full = place(axis_name, piece_rows, full, sum((near[j] for j in group), []), f"near_{k}")
        for k, group in enumerate(FAR_GROUPS):
            full = place(axis_name, piece_rows, full, sum((far[j] for j in group), []), f"far_{k}",
                         direct=True)

        grad_vec = grad_vec.reshape(-1)[:vec_size]
        new_p_vec, new_m_vec, new_v_vec = adam_update(grad_vec * clip[0, 0], p_vec, m_vec, v_vec, learn_rate, 0.0)
        new_p, new_m, new_v = (array.reshape(-1) for array in state)
        return new_p, new_m, new_v, new_p_vec, new_m_vec, new_v_vec, full.reshape(-1)

    return jax.shard_map(
        local_step,
        mesh=mesh,
        in_specs=(P(axis_name, None), P(axis_name, None), P(axis_name), P(axis_name), P(axis_name), P(), P(), P(), P()),
        out_specs=(P(axis_name), P(axis_name), P(axis_name), P(), P(), P(), P()),
        check_vma=False,
    )
```
